32 devices in a mesh: dp: 4 (over y, z), sp: 8 (over x, core).
Axes of the slice: x: 4, y: 2, z: 2, core: 2. Of those that a mesh axis runs over, the one named last changes fastest.
The devices are a block of a 4x4x8 slice.
Arguments:
- hidden: bfloat16 [4096, 2048], P(('dp', 'sp')), parts along dimension 0
- positions: int32 [4096], P(('dp', 'sp')), parts along dimension 0
- d_attn: bfloat16 [4096, 2048], P(('dp', 'sp')), parts along dimension 0
- ln_weight: bfloat16 [2048], replicated
- w_q: bfloat16 [2048, 2048], replicated
- w_k: bfloat16 [2048, 2048], replicated
- w_v: bfloat16 [2048, 2048], replicated
- w_o: bfloat16 [2048, 2048], replicated
Outputs:
- output 1: bfloat16 [4096, 2048], P(('dp', 'sp')), parts along dimension 0
- output 2: bfloat16 [4096, 2048], P(('dp', 'sp')), parts along dimension 0
- output 3: bfloat16 [8192], P('dp'), parts along dimension 0
- output 4: bfloat16 [8192, 2048], P('dp'), parts along dimension 0
- output 5: bfloat16 [8192, 2048], P('dp'), parts along dimension 0
- output 6: bfloat16 [8192, 2048], P('dp'), parts along dimension 0
- output 7: bfloat16 [8192, 2048], P('dp'), parts along dimension 0
There are 4 independent parts. The reference program is written for one: setup_inputs(seed, part) draws one part's arguments, and reference() takes and returns one part's arrays. A program takes and returns all parts, laid end to end along the dimension named above; an argument that names none is the same for every part.
All inputs are finite; a program needn't handle non-finite values.
Results may differ from the reference program's by a relative error of at most 0.0120283.
Values are sent between devices in bfloat16 or wider.
A program may use at most 768 MiB of HBM per device.

```python
import math
import jax
import jax.numpy as jnp
from jax import lax

MODEL_DIM = 2048
NUM_HEADS = 16
NUM_KV_HEADS = 16
HEAD_DIM = 128
SEQ_LEN = 1024
LN_EPS = 1e-5
ROPE_BASE = 10000.0
GROUP_SIZE = NUM_HEADS // NUM_KV_HEADS
ROW_BLOCK = math.gcd(SEQ_LEN, 64)
NUM_BLOCKS = SEQ_LEN // ROW_BLOCK
SCORE_SCALE = HEAD_DIM ** -0.5


def setup_inputs(seed: int = 0, part: int = 0) -> dict:
    base_key = jax.random.key(seed)
    part_keys = jax.random.split(jax.random.fold_in(base_key, part), 3)
    weight_keys = jax.random.split(base_key, 5)
    hidden = jax.random.normal(part_keys[0], (SEQ_LEN, MODEL_DIM), jnp.float32).astype(jnp.bfloat16)
    pos_steps = jax.random.randint(part_keys[1], (SEQ_LEN,), 1, 4, dtype=jnp.int32)
    positions = (jnp.cumsum(pos_steps) - pos_steps[0]).astype(jnp.int32)
    d_attn = jax.random.normal(part_keys[2], (SEQ_LEN, MODEL_DIM), jnp.float32).astype(jnp.bfloat16)
    ln_weight = (1.0 + 0.25 * jax.random.normal(weight_keys[0], (MODEL_DIM,), jnp.float32)).astype(jnp.bfloat16)
    q_scale = math.sqrt(math.log(SEQ_LEN) / MODEL_DIM)
    kv_scale = MODEL_DIM ** -0.5
    o_scale = (NUM_HEADS * HEAD_DIM) ** -0.5
    w_q = (jax.random.normal(weight_keys[1], (MODEL_DIM, NUM_HEADS * HEAD_DIM), jnp.float32) * q_scale).astype(jnp.bfloat16)
    w_k = (jax.random.normal(weight_keys[2], (MODEL_DIM, NUM_KV_HEADS * HEAD_DIM), jnp.float32) * kv_scale).astype(jnp.bfloat16)
    w_v = (jax.random.normal(weight_keys[3], (MODEL_DIM, NUM_KV_HEADS * HEAD_DIM), jnp.float32) * kv_scale).astype(jnp.bfloat16)
    w_o = (jax.random.normal(weight_keys[4], (NUM_HEADS * HEAD_DIM, MODEL_DIM), jnp.float32) * o_scale).astype(jnp.bfloat16)
    return {'hidden': hidden, 'positions': positions, 'd_attn': d_attn, 'ln_weight': ln_weight,
            'w_q': w_q, 'w_k': w_k, 'w_v': w_v, 'w_o': w_o}


def norm_f32(hid_f32, weight_f32):
    mean_val = jnp.mean(hid_f32, axis=-1, keepdims=True)
    centered = hid_f32 - mean_val
    var_val = jnp.mean(centered * centered, axis=-1, keepdims=True)
    return centered * lax.rsqrt(var_val + LN_EPS) * weight_f32


def rope_tables(positions):
    inv_freq = ROPE_BASE ** (-jnp.arange(0, HEAD_DIM, 2, dtype=jnp.float32) / HEAD_DIM)
    angles = positions.astype(jnp.float32)[:, None] * inv_freq[None, :]
    return jnp.cos(angles)[:, None, :], jnp.sin(angles)[:, None, :]


def apply_rope(values, cos_t, sin_t):
    rot_pairs = values.reshape(values.shape[:-1] + (HEAD_DIM // 2, 2))
    even_part = rot_pairs[..., 0]
    odd_part = rot_pairs[..., 1]
    new_even = even_part * cos_t - odd_part * sin_t
    new_odd = odd_part * cos_t + even_part * sin_t
    return jnp.stack([new_even, new_odd], axis=-1).reshape(values.shape)


def block_probs(q_f32, row_start, k_f32):
    scores = jnp.einsum('qgrd,kgd->grqk', q_f32, k_f32) * SCORE_SCALE
    row_ids = row_start + jnp.arange(ROW_BLOCK)
    col_ids = jnp.arange(SEQ_LEN)
    scores = jnp.where(row_ids[:, None] >= col_ids[None, :], scores, -jnp.inf)
    return jax.nn.softmax(scores, axis=-1)


def reference(hidden, positions, d_attn, ln_weight, w_q, w_k, w_v, w_o):
    normed32, norm_vjp = jax.vjp(norm_f32, hidden.astype(jnp.float32), ln_weight.astype(jnp.float32))
    normed = normed32.astype(jnp.bfloat16)
    cos_t, sin_t = rope_tables(positions)
    q_rot = apply_rope(jnp.dot(normed, w_q, preferred_element_type=jnp.float32).reshape(SEQ_LEN, NUM_HEADS, HEAD_DIM), cos_t, sin_t).astype(jnp.bfloat16)
    k_rot = apply_rope(jnp.dot(normed, w_k, preferred_element_type=jnp.float32).reshape(SEQ_LEN, NUM_KV_HEADS, HEAD_DIM), cos_t, sin_t).astype(jnp.bfloat16)
    v_all = jnp.dot(normed, w_v, preferred_element_type=jnp.float32).astype(jnp.bfloat16).reshape(SEQ_LEN, NUM_KV_HEADS, HEAD_DIM)
    q_grp = q_rot.reshape(NUM_BLOCKS, ROW_BLOCK, NUM_KV_HEADS, GROUP_SIZE, HEAD_DIM)
    k_f32 = k_rot.astype(jnp.float32)
    v_f32 = v_all.astype(jnp.float32)
    block_ids = jnp.arange(NUM_BLOCKS)

    def fwd_block(block_in):
        q_block, block_idx = block_in
        attn_prob = block_probs(q_block.astype(jnp.float32), block_idx * ROW_BLOCK, k_f32)
        prob_bf = attn_prob.astype(jnp.bfloat16).astype(jnp.float32)
        return jnp.einsum('grqk,kgd->qgrd', prob_bf, v_f32).astype(jnp.bfloat16)

    o_grp = lax.map(fwd_block, (q_grp, block_ids))
    o_tok = o_grp.reshape(SEQ_LEN, NUM_HEADS * HEAD_DIM)
    attn_out = jnp.dot(o_tok, w_o, preferred_element_type=jnp.float32).astype(jnp.bfloat16)
    d_o = jnp.dot(d_attn, w_o.T, preferred_element_type=jnp.float32).astype(jnp.bfloat16)
    dw_o = jnp.dot(o_tok.T, d_attn, preferred_element_type=jnp.float32)
    do_grp = d_o.reshape(NUM_BLOCKS, ROW_BLOCK, NUM_KV_HEADS, GROUP_SIZE, HEAD_DIM)

    def bwd_block(carry, block_in):
        dk_acc, dv_acc = carry
        q_block, do_block, block_idx = block_in
        q_f32 = q_block.astype(jnp.float32)
        do_f32 = do_block.astype(jnp.float32)
        attn_prob = block_probs(q_f32, block_idx * ROW_BLOCK, k_f32)
        prob_bf = attn_prob.astype(jnp.bfloat16).astype(jnp.float32)
        d_prob = jnp.einsum('qgrd,kgd->grqk', do_f32, v_f32)
        row_dot = jnp.sum(attn_prob * d_prob, axis=-1, keepdims=True)
        d_score = (attn_prob * (d_prob - row_dot) * SCORE_SCALE).astype(jnp.bfloat16).astype(jnp.float32)
        dq_block = jnp.einsum('grqk,kgd->qgrd', d_score, k_f32).astype(jnp.bfloat16)
        dk_acc = dk_acc + jnp.einsum('grqk,qgrd->kgd', d_score, q_f32)
        dv_acc = dv_acc + jnp.einsum('grqk,qgrd->kgd', prob_bf, do_f32)
        return (dk_acc, dv_acc), dq_block

    zero_acc = jnp.zeros((SEQ_LEN, NUM_KV_HEADS, HEAD_DIM), jnp.float32)
    kv_sums, dq_grp = lax.scan(bwd_block, (zero_acc, zero_acc), (q_grp, do_grp, block_ids))
    dk_bf = kv_sums[0].astype(jnp.bfloat16)
    dv_bf = kv_sums[1].astype(jnp.bfloat16)
    g_q = apply_rope(dq_grp.reshape(SEQ_LEN, NUM_HEADS, HEAD_DIM).astype(jnp.float32), cos_t, -sin_t).astype(jnp.bfloat16).reshape(SEQ_LEN, NUM_HEADS * HEAD_DIM)
    g_k = apply_rope(dk_bf.astype(jnp.float32), cos_t, -sin_t).astype(jnp.bfloat16).reshape(SEQ_LEN, NUM_KV_HEADS * HEAD_DIM)
    g_v = dv_bf.reshape(SEQ_LEN, NUM_KV_HEADS * HEAD_DIM)
    d_normed = (jnp.dot(g_q, w_q.T, preferred_element_type=jnp.float32)
                + jnp.dot(g_k, w_k.T, preferred_element_type=jnp.float32)
                + jnp.dot(g_v, w_v.T, preferred_element_type=jnp.float32))
    dw_q = jnp.dot(normed.T, g_q, preferred_element_type=jnp.float32)
    dw_k = jnp.dot(normed.T, g_k, preferred_element_type=jnp.float32)
    dw_v = jnp.dot(normed.T, g_v, preferred_element_type=jnp.float32)
    d_hid, d_lnw = norm_vjp(d_normed)
    return (attn_out, d_hid.astype(jnp.bfloat16), d_lnw.astype(jnp.bfloat16), dw_q.astype(jnp.bfloat16),
            dw_k.astype(jnp.bfloat16), dw_v.astype(jnp.bfloat16), dw_o.astype(jnp.bfloat16))
```

```python
import functools

import jax
import jax.numpy as jnp
from jax import lax
from jax.experimental import pallas as pl
from jax.experimental.pallas import tpu as pltpu
from jax.sharding import PartitionSpec as P

HEAD_DIM = 128
LN_EPS = 1e-5
ROPE_BASE = 10000.0
SCALE = HEAD_DIM ** -0.5
LOG2E = 1.4426950408889634
CORES = 2
QB = 256
MESH = pl.DeviceIdType.MESH
F32 = jnp.float32
BF16 = jnp.bfloat16


def norm_f32(hid_f32, weight_f32):
    mean_val = jnp.mean(hid_f32, axis=-1, keepdims=True)
    centered = hid_f32 - mean_val
    var_val = jnp.mean(centered * centered, axis=-1, keepdims=True)
    return centered * lax.rsqrt(var_val + LN_EPS) * weight_f32


def angle_table(positions):
    lane = jnp.arange(HEAD_DIM)
    inv_freq = ROPE_BASE ** (-((lane // 2) * 2).astype(F32) / HEAD_DIM)
    angles = positions.astype(F32)[:, None] * inv_freq[None, :]
    return jnp.where(lane[None, :] % 2 == 0, jnp.cos(angles), jnp.sin(angles))


def even_lanes(shape):
    return lax.broadcasted_iota(jnp.int32, shape, 1) % 2 == 0


def swap_pairs(y):
    return jnp.where(even_lanes(y.shape), pltpu.roll(y, HEAD_DIM - 1, 1), pltpu.roll(y, 1, 1))


def nt(a, b):
    return lax.dot_general(a, b, (((1,), (1,)), ((), ())), preferred_element_type=F32)


def main_kernel(n_dev, x_ref, g_ref, t_ref, w_ref, wq, wk, wv, wo,
                h_out, g_out, o_out, gq_out, gk_out, gv_out,
                h_all, g_all, t_all, cos_s, sin_s, w3, wo_s, qkv, do_s,
                res, dk_acc, dv_acc, kt_s, vt_s, pt_s, dst_s,
                ssem, rsem, wsem, lsem, xsem, osem):
    blk = x_ref.shape[0]
    half = blk // 2
    rows_chip = CORES * blk
    n_chips = n_dev // CORES
    heads = qkv.shape[1]
    width = heads * HEAD_DIM
    seq = n_dev * blk

    me = lax.axis_index("sp")
    chip, core = me // CORES, lax.rem(me, CORES)
    other = 1 - core

    def dev(step, cr):
        return lax.rem(chip + step + n_chips, n_chips) * CORES + cr

    partner, right, left = dev(0, other), dev(1, core), dev(-1, core)

    barrier = pltpu.get_barrier_semaphore()
    for d in (partner, right, left):
        pl.semaphore_signal(barrier, inc=1, device_id={"sp": d}, device_id_type=MESH)

    col0 = pl.multiple_of(core * width, width)
    wcopies = [
        pltpu.make_async_copy(w.at[:, pl.ds(col0, width)], w3.at[j], wsem.at[j])
        for j, w in enumerate((wq, wk, wv))
    ]
    wcopies.append(pltpu.make_async_copy(wo.at[pl.ds(col0, width), :], wo_s, wsem.at[3]))
    for c in wcopies:
        c.start()

    own = pl.ds(pl.multiple_of(me * blk, blk), blk)
    h_all[own, :] = norm_f32(x_ref[...].astype(F32), w_ref[...].astype(F32)).astype(BF16)
    g_all[own, :] = g_ref[...]
    t_all[own, :] = t_ref[...]

    arrays = (t_all, h_all, g_all)

    def region(block, piece):
        if piece is None:
            return pl.ds(pl.multiple_of(block * blk, blk), blk)
        return pl.ds(pl.multiple_of(block * blk + piece * half, half), half)

    def copy(a, kind, block, piece, to):
        r = region(block, piece)
        return pltpu.make_async_remote_copy(
            src_ref=arrays[a].at[r, :], dst_ref=arrays[a].at[r, :],
            send_sem=ssem.at[a, kind], recv_sem=rsem.at[a, kind],
            device_id={"sp": to}, device_id_type=MESH)

    far = 2
    sends = {
        0: (me, None, partner),
        1: (me, 0, right), 2: (me, 1, right),
        3: (me, 0, left), 4: (me, 1, left),
        5: (dev(-1, core), 0, right), 6: (dev(1, core), 1, left),
        7: (dev(-1, core), 0, partner), 8: (dev(-1, core), 1, partner),
        9: (dev(1, core), 0, partner), 10: (dev(1, core), 1, partner),
        11: (dev(far, core), 0, partner), 12: (dev(far, core), 1, partner),
    }
    recvs = {
        0: (partner, None),
        1: (dev(-1, core), 0), 2: (dev(-1, core), 1),
        3: (dev(1, core), 0), 4: (dev(1, core), 1),
        5: (dev(far, core), 0), 6: (dev(far, core), 1),
        7: (dev(-1, other), 0), 8: (dev(-1, other), 1),
        9: (dev(1, other), 0), 10: (dev(1, other), 1),
        11: (dev(far, other), 0), 12: (dev(far, other), 1),
    }

    def send(a, kind):
        block, piece, to = sends[kind]
        copy(a, kind, block, piece, to).start()

    def got(a, kind):
        block, piece = recvs[kind]
        copy(a, kind, block, piece, partner).wait_recv()

    pl.semaphore_wait(barrier, 3)
    for kind in (1, 2, 4, 3, 0):
        send(0, kind)
    for kind in (1, 4, 2, 3, 0):
        send(1, kind)
    send(2, 0)

    def pass_first(a):
        got(a, 1)
        send(a, 5)
        send(a, 7)
        got(a, 4)
        send(a, 6)
        send(a, 10)

    def pass_second(a):
        got(a, 2)
        send(a, 8)
        got(a, 3)
        send(a, 9)

    def pass_far(a):
        got(a, 5)
        send(a, 11)
        got(a, 6)
        send(a, 12)

    def from_partner(a, which):
        for kind in which:
            got(a, kind)

    def tables(step):
        r = pl.ds(pl.multiple_of(lax.rem(chip + step, n_chips) * rows_chip, rows_chip), rows_chip)
        t = t_all[r, :]
        even = even_lanes(t.shape)
        cos_s[r, :] = jnp.where(even, t, pltpu.roll(t, 1, 1))
        sin_s[r, :] = jnp.where(even, -pltpu.roll(t, HEAD_DIM - 1, 1), t)

    def project(step, j):
        r = pl.ds(pl.multiple_of(lax.rem(chip + step, n_chips) * rows_chip, rows_chip), rows_chip)
        y = jnp.dot(h_all[r, :], w3[j], preferred_element_type=F32)
        is_v = j == 2
        c = jnp.where(is_v, 1.0, cos_s[r, :])
        s = jnp.where(is_v, 0.0, sin_s[r, :])
        for n in range(heads):
            yn = y[:, n * HEAD_DIM:(n + 1) * HEAD_DIM]
            qkv[j, n, r, :] = (yn * c + swap_pairs(yn) * s).astype(BF16)

    def project_do(step):
        r = pl.ds(pl.multiple_of(lax.rem(chip + step, n_chips) * rows_chip, rows_chip), rows_chip)
        y = nt(g_all[r, :], wo_s[...])
        for n in range(heads):
            do_s[n, r, :] = y[:, n * HEAD_DIM:(n + 1) * HEAD_DIM].astype(BF16)

    got(0, 0)
    got(1, 0)
    tables(0)
    for c in wcopies:
        c.wait()

    @pl.loop(0, 3)
    def _(j):
        project(0, j)

    pass_first(0)
    pass_second(0)
    pass_far(0)
    pass_first(1)
    for kind in (1, 4, 2, 3):
        send(2, kind)
    pass_second(1)
    from_partner(0, (7, 8, 9, 10))
    from_partner(1, (7, 8, 9, 10))
    tables(1)
    tables(n_chips - 1)

    @pl.loop(0, 2)
    def _(i):
        @pl.loop(0, 3)
        def _(j):
            project(1 + i * (n_chips - 2), j)

    pass_far(1)
    from_partner(0, (11, 12))
    from_partner(1, (11, 12))
    tables(far)

    @pl.loop(0, 3)
    def _(j):
        project(far, j)

    h_copy = pltpu.make_async_copy(h_all, h_out, lsem.at[0])
    h_copy.start()
    got(2, 0)
    pass_first(2)
    pass_second(2)
    pass_far(2)
    from_partner(2, (7, 8, 9, 10, 11, 12))
    g_copy = pltpu.make_async_copy(g_all, g_out, lsem.at[1])
    g_copy.start()

    @pl.loop(0, n_chips)
    def _(i):
        project_do(i)

    c2 = SCALE * LOG2E
    outs = (o_out, gq_out, gk_out, gv_out)

    def out_copies(n):
        cols = pl.ds(pl.multiple_of(core * width + n * HEAD_DIM, HEAD_DIM), HEAD_DIM)
        local, remote = [], []
        for a in range(4):
            local.append(pltpu.make_async_copy(res.at[a, n], outs[a].at[:, cols], osem.at[a]))
            remote.append(pltpu.make_async_remote_copy(
                src_ref=res.at[a, n], dst_ref=outs[a].at[:, cols],
                send_sem=xsem.at[0, a], recv_sem=xsem.at[1, a],
                device_id={"sp": partner}, device_id_type=MESH))
        return local, remote

    @pl.loop(0, heads)
    def _(n):
        kt_s[...] = qkv[1, n].T
        vt_s[...] = qkv[2, n].T
        dk_acc[...] = jnp.zeros_like(dk_acc)
        dv_acc[...] = jnp.zeros_like(dv_acc)
        for i in range(seq // QB):
            L = (i + 1) * QB
            rq = slice(i * QB, L)
            q_i = qkv[0, n, rq, :]
            do_i = do_s[n, rq, :]
            s_t = nt(qkv[1, n, :L, :], q_i)
            key = lax.broadcasted_iota(jnp.int32, (QB, QB), 0)
            qry = lax.broadcasted_iota(jnp.int32, (QB, QB), 1)
            diag = jnp.where(key <= qry, s_t[i * QB:, :], -jnp.inf)
            s_t = diag if i == 0 else jnp.concatenate([s_t[:i * QB, :], diag], axis=0)
            m = jnp.max(s_t, axis=0, keepdims=True)
            e = jnp.exp2((s_t - m) * c2)
            p = e * (1.0 / jnp.sum(e, axis=0, keepdims=True))
            p_bf = p.astype(BF16)
            dp = nt(qkv[2, n, :L, :], do_i)
            rdot = jnp.sum(p * dp, axis=0, keepdims=True)
            ds = (p * (dp - rdot) * SCALE).astype(BF16)
            o_t = jnp.dot(vt_s[:, :L], p_bf, preferred_element_type=F32)
            res[0, n, rq, :] = o_t.T.astype(BF16)
            dq = jnp.dot(kt_s[:, :L], ds, preferred_element_type=F32).T.astype(BF16).astype(F32)
            res[1, n, rq, :] = (dq * cos_s[rq, :] - swap_pairs(dq) * sin_s[rq, :]).astype(BF16)
            dv_acc[:L, :] += jnp.dot(p_bf, do_i, preferred_element_type=F32)
            dk_acc[:L, :] += jnp.dot(ds, q_i, preferred_element_type=F32)
        dk = dk_acc[...].astype(BF16).astype(F32)
        res[2, n] = (dk * cos_s[...] - swap_pairs(dk) * sin_s[...]).astype(BF16)
        res[3, n] = dv_acc[...].astype(BF16)
        local, remote = out_copies(n)
        for c in local + remote:
            c.start()

    h_copy.wait()
    g_copy.wait()
    for a in range(3):
        for kind, (block, piece, to) in sends.items():
            copy(a, kind, block, piece, to).wait_send()
    mine = pl.ds(pl.multiple_of(core * width, width), width)
    theirs = pl.ds(pl.multiple_of(other * width, width), width)
    for a in range(4):
        pltpu.make_async_copy(outs[a].at[:, mine], outs[a].at[:, mine], osem.at[a]).wait()
        done = pltpu.make_async_remote_copy(
            src_ref=outs[a].at[:, mine], dst_ref=outs[a].at[:, theirs],
            send_sem=xsem.at[0, a], recv_sem=xsem.at[1, a],
            device_id={"sp": partner}, device_id_type=MESH)
        done.wait_send()
        done.wait_recv()


def run_main(n_dev, hidden, d_attn, table, ln_weight, w_q, w_k, w_v, w_o):
    blk, model = hidden.shape
    seq = n_dev * blk
    width = w_q.shape[1] // CORES
    heads = width // HEAD_DIM
    vm = pl.BlockSpec(memory_space=pltpu.VMEM)
    hbm = pl.BlockSpec(memory_space=pl.ANY)
    full = jax.ShapeDtypeStruct((seq, model), BF16)
    wide = jax.ShapeDtypeStruct((seq, w_q.shape[1]), BF16)
    return pl.pallas_call(
        functools.partial(main_kernel, n_dev),
        out_shape=(full, full, wide, wide, wide, wide),
        in_specs=[vm] * 4 + [hbm] * 4,
        out_specs=[hbm] * 6,
        scratch_shapes=[
            pltpu.VMEM((seq, model), BF16),
            pltpu.VMEM((seq, model), BF16),
            pltpu.VMEM((seq, HEAD_DIM), F32),
            pltpu.VMEM((seq, HEAD_DIM), F32),
            pltpu.VMEM((seq, HEAD_DIM), F32),
            pltpu.VMEM((3, model, width), BF16),
            pltpu.VMEM((width, model), BF16),
            pltpu.VMEM((3, heads, seq, HEAD_DIM), BF16),
            pltpu.VMEM((heads, seq, HEAD_DIM), BF16),
            pltpu.VMEM((4, heads, seq, HEAD_DIM), BF16),
            pltpu.VMEM((seq, HEAD_DIM), F32),
            pltpu.VMEM((seq, HEAD_DIM), F32),
            pltpu.VMEM((HEAD_DIM, seq), BF16),
            pltpu.VMEM((HEAD_DIM, seq), BF16),
            pltpu.VMEM((8, 128), BF16),
            pltpu.VMEM((8, 128), BF16),
            pltpu.SemaphoreType.DMA((3, 13)),
            pltpu.SemaphoreType.DMA((3, 13)),
            pltpu.SemaphoreType.DMA((4,)),
            pltpu.SemaphoreType.DMA((2,)),
            pltpu.SemaphoreType.DMA((2, 4)),
            pltpu.SemaphoreType.DMA((4,)),
        ],
        compiler_params=pltpu.CompilerParams(
            collective_id=0, has_side_effects=True, vmem_limit_bytes=67043328),
        name="gather_attention",
    )(hidden, d_attn, table, ln_weight.reshape(1, -1), w_q, w_k, w_v, w_o)


def solution(mesh):
    n_dev = mesh.shape['sp']
    row_spec = P(('dp', 'sp'), None)
    full_spec = P(None, None)
    grad_spec = P('dp', None)

    def local_step(hidden, positions, d_attn, ln_weight, w_q, w_k, w_v, w_o):
        blk = hidden.shape[0]
        table = angle_table(positions)
        h, g, o, gq, gk, gv = run_main(n_dev, hidden, d_attn, table, ln_weight, w_q, w_k, w_v, w_o)
        row0 = lax.axis_index('sp') * blk

        def mine(a):
            return lax.dynamic_slice_in_dim(a, row0, blk, 0)

        def tn(a, b):
            return lax.dot_general(a, b, (((0,), (0,)), ((), ())), preferred_element_type=F32).astype(BF16)

        attn_out = jnp.dot(mine(o), w_o, preferred_element_type=F32).astype(BF16)
        dh = (jnp.einsum('te,de->td', mine(gq), w_q, preferred_element_type=F32)
              + jnp.einsum('te,de->td', mine(gk), w_k, preferred_element_type=F32)
              + jnp.einsum('te,de->td', mine(gv), w_v, preferred_element_type=F32))
        _, norm_vjp = jax.vjp(norm_f32, hidden.astype(F32), ln_weight.astype(F32))
        d_hid, d_lnw = norm_vjp(dh)
        d_lnw = lax.psum(d_lnw, 'sp').astype(BF16)
        return (attn_out, d_hid.astype(BF16), d_lnw, tn(h, gq), tn(h, gk), tn(h, gv), tn(o, g))

    return jax.shard_map(local_step, mesh=mesh,
                         in_specs=(row_spec, P(('dp', 'sp')), row_spec, P(None), full_spec, full_spec, full_spec, full_spec),
                         out_specs=(row_spec, row_spec, P('dp'), grad_spec, grad_spec, grad_spec, grad_spec),
                         check_vma=False)
```

```python
import functools

import jax
import jax.numpy as jnp
from jax import lax
from jax.experimental import pallas as pl
from jax.experimental.pallas import tpu as pltpu
from jax.sharding import PartitionSpec as P

HEAD_DIM = 128
LN_EPS = 1e-5
ROPE_BASE = 10000.0
SCALE = HEAD_DIM ** -0.5
LOG2E = 1.4426950408889634
CORES = 2
QB = 256
MT = 256
VMEM_LIMIT = 67043328
MESH = pl.DeviceIdType.MESH
F32 = jnp.float32
BF16 = jnp.bfloat16


def normalize(x):
    x = x.astype(F32)
    centered = x - jnp.mean(x, axis=-1, keepdims=True)
    rstd = lax.rsqrt(jnp.mean(centered * centered, axis=-1, keepdims=True) + LN_EPS)
    return centered * rstd, rstd


def sin_cos(a):
    n = jnp.floor(a * 0.6366197723675814 + 0.5)
    r = ((a - n * 1.5703125) - n * 4.8375129699707031e-4) - n * 7.5497899548918821e-8
    z = r * r
    s = r + r * z * (-1.6666654611e-1 + z * (8.3321608736e-3 + z * -1.9515295891e-4))
    c = 1.0 - 0.5 * z + z * z * (4.166664568298827e-2 + z * (-1.388731625493765e-3 + z * 2.443315711809948e-5))
    quad = n.astype(jnp.int32)
    odd = (quad & 1) == 1
    sin = jnp.where(odd, c, s)
    cos = jnp.where(odd, s, c)
    return jnp.where((quad & 2) == 2, -sin, sin), jnp.where(((quad + 1) & 2) == 2, -cos, cos)


def even_lanes(shape):
    return lax.broadcasted_iota(jnp.int32, shape, 1) % 2 == 0


def swap_pairs(y):
    return jnp.where(even_lanes(y.shape), pltpu.roll(y, HEAD_DIM - 1, 1), pltpu.roll(y, 1, 1))


def nt(a, b):
    return lax.dot_general(a, b, (((1,), (1,)), ((), ())), preferred_element_type=F32)


def nn(a, b):
    return jnp.dot(a, b, preferred_element_type=F32)


def main_kernel(n_dev, x_ref, g_ref, p_ref, f_ref, w_ref, wq, wk, wv, wo,
                h_out, g_out, o_out, gq_out, gk_out, gv_out, a_out, dx_out, dl_out,
                h_all, g_all, pos, cos_s, sin_s, w3, wo_s, qkv, do_s,
                res, m_s, li_s, kt_s, vt_s, pt_s, dst_s, a_part, a_recv, dh_part, dh_recv, dl_buf,
                ssem, rsem, wsem, lsem, xsem, osem, psem, dsem, fsem):
    blk, model = x_ref.shape
    half = blk // 2
    rows_chip = CORES * blk
    n_chips = n_dev // CORES
    heads = qkv.shape[1]
    width = heads * HEAD_DIM
    seq = n_dev * blk
    nq = seq // QB

    me = lax.axis_index("sp")
    chip, core = me // CORES, lax.rem(me, CORES)
    other = 1 - core

    def dev(step, cr):
        return lax.rem(chip + step + n_chips, n_chips) * CORES + cr

    partner, right, left = dev(0, other), dev(1, core), dev(-1, core)
    others = [lax.rem(me + k, n_dev) for k in range(1, n_dev)]

    barrier = pltpu.get_barrier_semaphore()
    for d in others:
        pl.semaphore_signal(barrier, inc=1, device_id={"sp": d}, device_id_type=MESH)

    col0 = pl.multiple_of(core * width, width)
    wcopies = [
        pltpu.make_async_copy(w.at[:, pl.ds(col0, width)], w3.at[j], wsem.at[j])
        for j, w in enumerate((wq, wk, wv))
    ]
    wcopies.append(pltpu.make_async_copy(wo.at[pl.ds(col0, width), :], wo_s, wsem.at[3]))
    for c in wcopies:
        c.start()

    own = pl.ds(pl.multiple_of(me * blk, blk), blk)
    ln_w = w_ref[...].astype(F32).reshape(1, model)
    h_all[own, :] = (normalize(x_ref[...])[0] * ln_w).astype(BF16)
    g_all[own, :] = g_ref[...]
    pos[me] = p_ref[...].reshape(1, blk)

    arrays = (h_all, g_all)

    def region(block, piece):
        if piece is None:
            return pl.ds(pl.multiple_of(block * blk, blk), blk)
        return pl.ds(pl.multiple_of(block * blk + piece * half, half), half)

    def copy(a, kind, block, piece, to):
        r = region(block, piece)
        return pltpu.make_async_remote_copy(
            src_ref=arrays[a].at[r, :], dst_ref=arrays[a].at[r, :],
            send_sem=ssem.at[a, kind], recv_sem=rsem.at[a, kind],
            device_id={"sp": to}, device_id_type=MESH)

    far = 2
    sends = {
        0: (me, None, partner),
        1: (me, 0, right), 2: (me, 1, right),
        3: (me, 0, left), 4: (me, 1, left),
        5: (dev(-1, core), 0, right), 6: (dev(1, core), 1, left),
        7: (dev(-1, core), 0, partner), 8: (dev(-1, core), 1, partner),
        9: (dev(1, core), 0, partner), 10: (dev(1, core), 1, partner),
        11: (dev(far, core), 0, partner), 12: (dev(far, core), 1, partner),
    }
    recvs = {
        0: (partner, None),
        1: (dev(-1, core), 0), 2: (dev(-1, core), 1),
        3: (dev(1, core), 0), 4: (dev(1, core), 1),
        5: (dev(far, core), 0), 6: (dev(far, core), 1),
        7: (dev(-1, other), 0), 8: (dev(-1, other), 1),
        9: (dev(1, other), 0), 10: (dev(1, other), 1),
        11: (dev(far, other), 0), 12: (dev(far, other), 1),
    }

    def send(a, kind):
        block, piece, to = sends[kind]
        copy(a, kind, block, piece, to).start()

    def got(a, kind):
        block, piece = recvs[kind]
        copy(a, kind, block, piece, partner).wait_recv()

    def small(buf, sems, k, source, to):
        return pltpu.make_async_remote_copy(
            src_ref=buf.at[source], dst_ref=buf.at[source],
            send_sem=sems.at[0, k], recv_sem=sems.at[1, k],
            device_id={"sp": to}, device_id_type=MESH)

    def small_send(buf, sems):
        for k in range(1, n_dev):
            small(buf, sems, k, me, others[k - 1]).start()

    def small_wait(buf, sems):
        for k in range(1, n_dev):
            small(buf, sems, k, lax.rem(me - k + n_dev, n_dev), partner).wait_recv()
        for k in range(1, n_dev):
            small(buf, sems, k, me, partner).wait_send()

    pl.semaphore_wait(barrier, n_dev - 1)
    for kind in (1, 4, 2, 3, 0):
        send(0, kind)
    small_send(pos, psem)
    send(1, 0)

    def pass_first(a):
        got(a, 1)
        send(a, 5)
        send(a, 7)
        got(a, 4)
        send(a, 6)
        send(a, 10)

    def pass_second(a):
        got(a, 2)
        send(a, 8)
        got(a, 3)
        send(a, 9)

    def pass_far(a):
        got(a, 5)
        send(a, 11)
        got(a, 6)
        send(a, 12)

    def from_partner(a, which):
        for kind in which:
            got(a, kind)

    def chip_rows(i):
        step = lax.rem(i * (i + 1) // 2, n_chips)
        return pl.ds(pl.multiple_of(lax.rem(chip + step, n_chips) * rows_chip, rows_chip), rows_chip)

    def fill_tables():
        small_wait(pos, psem)
        diag = (lax.broadcasted_iota(jnp.int32, (blk, blk), 0)
                == lax.broadcasted_iota(jnp.int32, (blk, blk), 1))
        even = even_lanes((blk, HEAD_DIM))

        @pl.loop(0, n_dev)
        def _(b):
            r = pl.ds(pl.multiple_of(b * blk, blk), blk)
            p = jnp.broadcast_to(pos[b].astype(F32), (blk, blk))
            col = jnp.sum(jnp.where(diag, p, 0.0), axis=1, keepdims=True)
            sin, cos = sin_cos(col * f_ref[...])
            cos_s[r, :] = cos
            sin_s[r, :] = jnp.where(even, -sin, sin)

    @pl.loop(0, 3 * n_chips)
    def _(it):
        i, j = it // 3, lax.rem(it, 3)

        @pl.when(it == 0)
        def _():
            fill_tables()
            got(0, 0)
            for c in wcopies:
                c.wait()

        @pl.when(it == 3)
        def _():
            pass_first(0)
            for kind in (1, 4, 2, 3):
                send(1, kind)
            pass_second(0)
            from_partner(0, (7, 8, 9, 10))

        @pl.when(it == 9)
        def _():
            pass_far(0)
            from_partner(0, (11, 12))

        r = chip_rows(i)
        y = nn(h_all[r, :], w3[j])
        is_v = j == 2
        c = jnp.where(is_v, 1.0, cos_s[r, :])
        s = jnp.where(is_v, 0.0, sin_s[r, :])
        for n in range(heads):
            yn = y[:, n * HEAD_DIM:(n + 1) * HEAD_DIM]
            qkv[j, n, r, :] = (yn * c + swap_pairs(yn) * s).astype(BF16)

    h_copy = pltpu.make_async_copy(h_all, h_out, lsem.at[0])
    h_copy.start()

    outs = (o_out, gq_out, gk_out, gv_out)

    def send_head(a, n):
        cols = pl.ds(pl.multiple_of(core * width + n * HEAD_DIM, HEAD_DIM), HEAD_DIM)
        pltpu.make_async_copy(res.at[a, n], outs[a].at[:, cols], osem.at[a]).start()
        pltpu.make_async_remote_copy(
            src_ref=res.at[a, n], dst_ref=outs[a].at[:, cols],
            send_sem=xsem.at[0, a], recv_sem=xsem.at[1, a],
            device_id={"sp": partner}, device_id_type=MESH).start()

    c2 = SCALE * LOG2E
    causal = (lax.broadcasted_iota(jnp.int32, (QB, QB), 0)
              <= lax.broadcasted_iota(jnp.int32, (QB, QB), 1))

    def tile(i):
        return slice(i * QB, (i + 1) * QB)

    def scores(n, i, j):
        s = nt(qkv[1, n, tile(j), :], qkv[0, n, tile(i), :])
        return jnp.where(causal, s, -jnp.inf) if i == j else s

    @pl.loop(0, heads)
    def _(n):
        @pl.when(n == 2)
        def _():
            got(1, 0)
            pass_first(1)

        vt_s[...] = qkv[2, n].T
        for i in range(nq):
            ss = [scores(n, i, j) for j in range(i + 1)]
            m = functools.reduce(jnp.maximum, [jnp.max(s, axis=0, keepdims=True) for s in ss])
            es = [jnp.exp2((s - m) * c2) for s in ss]
            li = 1.0 / sum(jnp.sum(e, axis=0, keepdims=True) for e in es)
            m_s[n, :, tile(i)] = m
            li_s[n, :, tile(i)] = li
            o_t = sum(nn(vt_s[:, tile(j)], (e * li).astype(BF16)) for j, e in enumerate(es))
            res[0, n, tile(i), :] = o_t.T.astype(BF16)
        send_head(0, n)

    @pl.loop(0, n_chips)
    def _(i):
        @pl.when(i == 1)
        def _():
            pass_second(1)
            from_partner(1, (7, 8, 9, 10))

        @pl.when(i == 3)
        def _():
            pass_far(1)
            from_partner(1, (11, 12))

        r = chip_rows(i)
        y = nt(g_all[r, :], wo_s[...])
        for n in range(heads):
            do_s[n, r, :] = y[:, n * HEAD_DIM:(n + 1) * HEAD_DIM].astype(BF16)

    g_copy = pltpu.make_async_copy(g_all, g_out, lsem.at[1])
    g_copy.start()

    def rows_of(a, r):
        return jnp.concatenate([res[a, n, r, :] for n in range(heads)], axis=1)

    here = pl.ds(pl.multiple_of(chip * rows_chip, rows_chip), rows_chip)
    mine = pl.ds(pl.multiple_of(core * blk, blk), blk)
    theirs = pl.ds(pl.multiple_of(other * blk, blk), blk)

    def swap_part(part, recv, k):
        return pltpu.make_async_remote_copy(
            src_ref=part.at[theirs, :], dst_ref=recv,
            send_sem=fsem.at[0, k], recv_sem=fsem.at[1, k],
            device_id={"sp": partner}, device_id_type=MESH)

    a_part[...] = nn(rows_of(0, here), wo_s[...])
    a_swap = swap_part(a_part, a_recv, 0)
    a_swap.start()

    @pl.loop(0, heads)
    def _(n):
        kt_s[...] = qkv[1, n].T
        for i in range(nq):
            q_i, do_i = qkv[0, n, tile(i), :], do_s[n, tile(i), :]
            m, li = m_s[n, :, tile(i)], li_s[n, :, tile(i)]
            ps, dps = [], []
            rdot = 0.0
            for j in range(i + 1):
                p = jnp.exp2((scores(n, i, j) - m) * c2) * li
                dp = nt(qkv[2, n, tile(j), :], do_i)
                rdot = rdot + jnp.sum(p * dp, axis=0, keepdims=True)
                pt_s[tile(j), tile(i)] = p.astype(BF16)
                ps.append(p)
                dps.append(dp)
            for j in range(i + 1):
                dst_s[tile(j), tile(i)] = (ps[j] * (dps[j] - rdot) * SCALE).astype(BF16)
            dq = nn(kt_s[:, :(i + 1) * QB], dst_s[:(i + 1) * QB, tile(i)]).T.astype(BF16).astype(F32)
            res[1, n, tile(i), :] = (dq * cos_s[tile(i), :] - swap_pairs(dq) * sin_s[tile(i), :]).astype(BF16)
        for j in range(nq):
            dk = nn(dst_s[tile(j), j * QB:], qkv[0, n, j * QB:, :]).astype(BF16).astype(F32)
            res[2, n, tile(j), :] = (dk * cos_s[tile(j), :] - swap_pairs(dk) * sin_s[tile(j), :]).astype(BF16)
            res[3, n, tile(j), :] = nn(pt_s[tile(j), j * QB:], do_s[n, j * QB:, :]).astype(BF16)
        for a in (1, 2, 3):
            send_head(a, n)

    dh_part[...] = sum(nt(rows_of(j + 1, here), w3[j]) for j in range(3))
    dh_swap = swap_part(dh_part, dh_recv, 1)
    dh_swap.start()
    a_swap.wait()
    a_out[...] = (a_part[mine, :] + a_recv[...]).astype(BF16)
    xhat, rstd = normalize(x_ref[...])
    dh_swap.wait()
    dh = dh_part[mine, :] + dh_recv[...]
    dl_buf[me] = jnp.sum(dh * xhat, axis=0, keepdims=True)
    small_send(dl_buf, dsem)
    dy = dh * ln_w
    dx = dy - jnp.mean(dy, axis=-1, keepdims=True) - xhat * jnp.mean(dy * xhat, axis=-1, keepdims=True)
    dx_out[...] = (dx * rstd).astype(BF16)

    h_copy.wait()
    g_copy.wait()
    for a in range(2):
        for kind, (block, piece, to) in sends.items():
            copy(a, kind, block, piece, to).wait_send()
    my_cols = pl.ds(pl.multiple_of(core * width, width), width)
    their_cols = pl.ds(pl.multiple_of(other * width, width), width)
    for a in range(4):
        pltpu.make_async_copy(outs[a].at[:, my_cols], outs[a].at[:, my_cols], osem.at[a]).wait()
        done = pltpu.make_async_remote_copy(
            src_ref=outs[a].at[:, my_cols], dst_ref=outs[a].at[:, their_cols],
            send_sem=xsem.at[0, a], recv_sem=xsem.at[1, a],
            device_id={"sp": partner}, device_id_type=MESH)
        done.wait_send()
        done.wait_recv()
    small_wait(dl_buf, dsem)
    total = dl_buf[0]
    for k in range(1, n_dev):
        total = total + dl_buf[k]
    dl_out[...] = total.astype(BF16).reshape(model)


def run_main(n_dev, hidden, d_attn, positions, ln_weight, w_q, w_k, w_v, w_o):
    blk, model = hidden.shape
    seq = n_dev * blk
    width = w_q.shape[1] // CORES
    heads = width // HEAD_DIM
    vm = pl.BlockSpec(memory_space=pltpu.VMEM)
    hbm = pl.BlockSpec(memory_space=pl.ANY)
    full = jax.ShapeDtypeStruct((seq, model), BF16)
    wide = jax.ShapeDtypeStruct((seq, w_q.shape[1]), BF16)
    rows = jax.ShapeDtypeStruct((blk, model), BF16)
    freq = jnp.repeat(ROPE_BASE ** (-jnp.arange(0, HEAD_DIM, 2, dtype=F32) / HEAD_DIM), 2)[None, :]
    return pl.pallas_call(
        functools.partial(main_kernel, n_dev),
        out_shape=(full, full, wide, wide, wide, wide, rows, rows, jax.ShapeDtypeStruct((model,), BF16)),
        in_specs=[vm] * 5 + [hbm] * 4,
        out_specs=[hbm] * 6 + [vm] * 3,
        scratch_shapes=[
            pltpu.VMEM((seq, model), BF16),
            pltpu.VMEM((seq, model), BF16),
            pltpu.VMEM((n_dev, 1, blk), jnp.int32),
            pltpu.VMEM((seq, HEAD_DIM), F32),
            pltpu.VMEM((seq, HEAD_DIM), F32),
            pltpu.VMEM((3, model, width), BF16),
            pltpu.VMEM((width, model), BF16),
            pltpu.VMEM((3, heads, seq, HEAD_DIM), BF16),
            pltpu.VMEM((heads, seq, HEAD_DIM), BF16),
            pltpu.VMEM((4, heads, seq, HEAD_DIM), BF16),
            pltpu.VMEM((heads, 1, seq), F32),
            pltpu.VMEM((heads, 1, seq), F32),
            pltpu.VMEM((HEAD_DIM, seq), BF16),
            pltpu.VMEM((HEAD_DIM, seq), BF16),
            pltpu.VMEM((seq, seq), BF16),
            pltpu.VMEM((seq, seq), BF16),
            pltpu.VMEM((CORES * blk, model), F32),
            pltpu.VMEM((blk, model), F32),
            pltpu.VMEM((CORES * blk, model), F32),
            pltpu.VMEM((blk, model), F32),
            pltpu.VMEM((n_dev, 1, model), F32),
            pltpu.SemaphoreType.DMA((2, 13)),
            pltpu.SemaphoreType.DMA((2, 13)),
            pltpu.SemaphoreType.DMA((4,)),
            pltpu.SemaphoreType.DMA((2,)),
            pltpu.SemaphoreType.DMA((2, 4)),
            pltpu.SemaphoreType.DMA((4,)),
            pltpu.SemaphoreType.DMA((2, n_dev)),
            pltpu.SemaphoreType.DMA((2, n_dev)),
            pltpu.SemaphoreType.DMA((2, 2)),
        ],
        compiler_params=pltpu.CompilerParams(
            collective_id=0, has_side_effects=True, vmem_limit_bytes=VMEM_LIMIT),
        name="gather_attention",
    )(hidden, d_attn, positions, freq, ln_weight, w_q, w_k, w_v, w_o)


def grad_kernel(h_ref, o_ref, gq, gk, gv, g, dq_ref, dk_ref, dv_ref, do_ref, rhs, sem):
    w, m = pl.program_id(0), pl.program_id(1)

    def load(k):
        src = (gq, gk, gv, g)[k]
        return pltpu.make_async_copy(src, rhs.at[k % 2], sem.at[k % 2])

    for k in range(4):
        @pl.when((w == k) & (m == 0))
        def _():
            if k == 0:
                load(0).start()
            load(k).wait()
            if k < 3:
                load(k + 1).start()

    def tn(a):
        b = rhs[lax.rem(w, 2)]
        return lax.dot_general(a, b, (((0,), (0,)), ((), ())), preferred_element_type=F32).astype(BF16)

    for k, out in enumerate((dq_ref, dk_ref, dv_ref, do_ref)):
        @pl.when(w == k)
        def _():
            out[...] = tn(o_ref[...] if k == 3 else h_ref[...])


def run_grads(h, o, gq, gk, gv, g):
    seq, model = h.shape
    wide = gq.shape[1]
    steps = model // MT
    hbm = pl.BlockSpec(memory_space=pl.ANY)

    def out_spec(k):
        return pl.BlockSpec((MT, wide), lambda w, m: (jnp.where(w == k, m, jnp.where(w < k, 0, steps - 1)), 0))

    return pl.pallas_call(
        grad_kernel,
        grid=(4, steps),
        out_shape=[jax.ShapeDtypeStruct((model, wide), BF16)] * 4,
        in_specs=[
            pl.BlockSpec((seq, MT), lambda w, m: (0, jnp.where(w < 3, m, steps - 1))),
            pl.BlockSpec((seq, MT), lambda w, m: (0, jnp.where(w < 3, 0, m))),
            hbm, hbm, hbm, hbm],
        out_specs=[out_spec(k) for k in range(4)],
        scratch_shapes=[pltpu.VMEM((2, seq, wide), BF16), pltpu.SemaphoreType.DMA((2,))],
        compiler_params=pltpu.CompilerParams(
            dimension_semantics=("arbitrary", "arbitrary"), vmem_limit_bytes=VMEM_LIMIT),
        name="weight_grads",
    )(h, o, gq, gk, gv, g)


def solution(mesh):
    n_dev = mesh.shape['sp']
    row_spec = P(('dp', 'sp'), None)
    full_spec = P(None, None)
    grad_spec = P('dp', None)

    def local_step(hidden, positions, d_attn, ln_weight, w_q, w_k, w_v, w_o):
        h, g, o, gq, gk, gv, attn_out, d_hid, d_lnw = run_main(
            n_dev, hidden, d_attn, positions, ln_weight, w_q, w_k, w_v, w_o)
        return (attn_out, d_hid, d_lnw, *run_grads(h, o, gq, gk, gv, g))

    return jax.shard_map(local_step, mesh=mesh,
                         in_specs=(row_spec, P(('dp', 'sp')), row_spec, P(None), full_spec, full_spec, full_spec, full_spec),
                         out_specs=(row_spec, row_spec, P('dp'), grad_spec, grad_spec, grad_spec, grad_spec),
                         check_vma=False)
```

```python
import functools

import jax
import jax.numpy as jnp
from jax import lax
from jax.experimental import pallas as pl
from jax.experimental.pallas import tpu as pltpu
from jax.sharding import PartitionSpec as P

HEAD_DIM = 128
LN_EPS = 1e-5
ROPE_BASE = 10000.0
SCALE = HEAD_DIM ** -0.5
LOG2E = 1.4426950408889634
CORES = 2
QB = 256
MT = 512
NT = 1024
VMEM_LIMIT = 67043328
MESH = pl.DeviceIdType.MESH
F32 = jnp.float32
BF16 = jnp.bfloat16


def normalize(x):
    x = x.astype(F32)
    centered = x - jnp.mean(x, axis=-1, keepdims=True)
    rstd = lax.rsqrt(jnp.mean(centered * centered, axis=-1, keepdims=True) + LN_EPS)
    return centered * rstd, rstd


def sin_cos(a):
    n = jnp.floor(a * 0.6366197723675814 + 0.5)
    r = ((a - n * 1.5703125) - n * 4.8375129699707031e-4) - n * 7.5497899548918821e-8
    z = r * r
    s = r + r * z * (-1.6666654611e-1 + z * (8.3321608736e-3 + z * -1.9515295891e-4))
    c = 1.0 - 0.5 * z + z * z * (4.166664568298827e-2 + z * (-1.388731625493765e-3 + z * 2.443315711809948e-5))
    quad = n.astype(jnp.int32)
    odd = (quad & 1) == 1
    sin = jnp.where(odd, c, s)
    cos = jnp.where(odd, s, c)
    return jnp.where((quad & 2) == 2, -sin, sin), jnp.where(((quad + 1) & 2) == 2, -cos, cos)


def even_lanes(shape):
    return lax.broadcasted_iota(jnp.int32, shape, 1) % 2 == 0


def swap_pairs(y):
    return jnp.where(even_lanes(y.shape), pltpu.roll(y, HEAD_DIM - 1, 1), pltpu.roll(y, 1, 1))


def nt(a, b):
    return lax.dot_general(a, b, (((1,), (1,)), ((), ())), preferred_element_type=F32)


def nn(a, b):
    return jnp.dot(a, b, preferred_element_type=F32)


def main_kernel(n_dev, x_ref, g_ref, p_ref, f_ref, w_ref, wq, wk, wv, wo,
                h_out, g_out, ot_out, gq_out, gk_out, gv_out, a_out, dx_out, dl_out,
                h_all, g_all, pos, cos_s, sin_s, w3, wo_s, wot_s, qkv, do_s,
                ot_s, res, m_s, li_s, kt_s, vt_s, pt_s, dst_s, a_part, a_recv, dh_part, dh_recv, cols_s, dl_buf,
                ssem, rsem, wsem, lsem, xsem, osem, psem, dsem, fsem):
    blk, model = x_ref.shape
    half = blk // 2
    rows_chip = CORES * blk
    n_chips = n_dev // CORES
    heads = qkv.shape[1]
    width = heads * HEAD_DIM
    seq = n_dev * blk
    nq = seq // QB

    me = lax.axis_index("sp")
    chip, core = me // CORES, lax.rem(me, CORES)
    other = 1 - core

    def dev(step, cr):
        return lax.rem(chip + step + n_chips, n_chips) * CORES + cr

    partner, right, left = dev(0, other), dev(1, core), dev(-1, core)
    others = [lax.rem(me + k, n_dev) for k in range(1, n_dev)]

    barrier = pltpu.get_barrier_semaphore()
    for d in others:
        pl.semaphore_signal(barrier, inc=1, device_id={"sp": d}, device_id_type=MESH)

    col0 = pl.multiple_of(core * width, width)
    wcopies = [
        pltpu.make_async_copy(w.at[:, pl.ds(col0, width)], w3.at[j], wsem.at[j])
        for j, w in enumerate((wq, wk, wv))
    ]
    wcopies.append(pltpu.make_async_copy(wo.at[pl.ds(col0, width), :], wo_s, wsem.at[3]))
    for c in wcopies:
        c.start()

    own = pl.ds(pl.multiple_of(me * blk, blk), blk)
    ln_w = w_ref[...].astype(F32).reshape(1, model)
    h_all[own, :] = (normalize(x_ref[...])[0] * ln_w).astype(BF16)
    g_all[own, :] = g_ref[...]
    pos[me] = p_ref[...].reshape(1, blk)

    arrays = (h_all, g_all)

    def region(block, piece):
        if piece is None:
            return pl.ds(pl.multiple_of(block * blk, blk), blk)
        return pl.ds(pl.multiple_of(block * blk + piece * half, half), half)

    def copy(a, kind, block, piece, to):
        r = region(block, piece)
        return pltpu.make_async_remote_copy(
            src_ref=arrays[a].at[r, :], dst_ref=arrays[a].at[r, :],
            send_sem=ssem.at[a, kind], recv_sem=rsem.at[a, kind],
            device_id={"sp": to}, device_id_type=MESH)

    far = 2
    sends = {
        0: (me, None, partner),
        1: (me, 0, right), 2: (me, 1, right),
        3: (me, 0, left), 4: (me, 1, left),
        5: (dev(-1, core), 0, right), 6: (dev(1, core), 1, left),
        7: (dev(-1, core), 0, partner), 8: (dev(-1, core), 1, partner),
        9: (dev(1, core), 0, partner), 10: (dev(1, core), 1, partner),
        11: (dev(far, core), 0, partner), 12: (dev(far, core), 1, partner),
    }
    recvs = {
        0: (partner, None),
        1: (dev(-1, core), 0), 2: (dev(-1, core), 1),
        3: (dev(1, core), 0), 4: (dev(1, core), 1),
        5: (dev(far, core), 0), 6: (dev(far, core), 1),
        7: (dev(-1, other), 0), 8: (dev(-1, other), 1),
        9: (dev(1, other), 0), 10: (dev(1, other), 1),
        11: (dev(far, other), 0), 12: (dev(far, other), 1),
    }

    def send(a, kind):
        block, piece, to = sends[kind]
        copy(a, kind, block, piece, to).start()

    def got(a, kind):
        block, piece = recvs[kind]
        copy(a, kind, block, piece, partner).wait_recv()

    def small(buf, sems, k, source, to):
        return pltpu.make_async_remote_copy(
            src_ref=buf.at[source], dst_ref=buf.at[source],
            send_sem=sems.at[0, k], recv_sem=sems.at[1, k],
            device_id={"sp": to}, device_id_type=MESH)

    def small_send(buf, sems):
        for k in range(1, n_dev):
            small(buf, sems, k, me, others[k - 1]).start()

    def small_wait(buf, sems):
        for k in range(1, n_dev):
            small(buf, sems, k, lax.rem(me - k + n_dev, n_dev), partner).wait_recv()
        for k in range(1, n_dev):
            small(buf, sems, k, me, partner).wait_send()

    pl.semaphore_wait(barrier, n_dev - 1)
    small_send(pos, psem)
    for kind in (1, 4, 2, 3, 0):
        send(0, kind)
    send(1, 0)

    def pass_first(a):
        got(a, 1)
        send(a, 5)
        send(a, 7)
        got(a, 4)
        send(a, 6)
        send(a, 10)

    def pass_second(a):
        got(a, 2)
        send(a, 8)
        got(a, 3)
        send(a, 9)

    def pass_far(a):
        got(a, 5)
        send(a, 11)
        got(a, 6)
        send(a, 12)

    def from_partner(a, which):
        for kind in which:
            got(a, kind)

    def chip_rows(i):
        step = lax.rem(i * (i + 1) // 2, n_chips)
        return pl.ds(pl.multiple_of(lax.rem(chip + step, n_chips) * rows_chip, rows_chip), rows_chip)

    def fill_tables():
        small_wait(pos, psem)
        diag = (lax.broadcasted_iota(jnp.int32, (blk, blk), 0)
                == lax.broadcasted_iota(jnp.int32, (blk, blk), 1))
        even = even_lanes((blk, HEAD_DIM))

        @pl.loop(0, n_dev)
        def _(b):
            r = pl.ds(pl.multiple_of(b * blk, blk), blk)
            p = jnp.broadcast_to(pos[b].astype(F32), (blk, blk))
            col = jnp.sum(jnp.where(diag, p, 0.0), axis=1, keepdims=True)
            sin, cos = sin_cos(col * f_ref[...])
            cos_s[r, :] = cos
            sin_s[r, :] = jnp.where(even, -sin, sin)

    @pl.loop(0, 3 * n_chips)
    def _(it):
        i, j = it // 3, lax.rem(it, 3)

        @pl.when(it == 0)
        def _():
            fill_tables()
            got(0, 0)
            for c in wcopies:
                c.wait()

        @pl.when(it == 3)
        def _():
            for e in range(width // QB):
                wot_s[:, e * QB:(e + 1) * QB] = wo_s[e * QB:(e + 1) * QB, :].T
            pass_first(0)
            for kind in (1, 4, 2, 3):
                send(1, kind)
            pass_second(0)
            from_partner(0, (7, 8, 9, 10))

        @pl.when(it == 9)
        def _():
            pass_far(0)
            from_partner(0, (11, 12))

        r = chip_rows(i)
        is_v = j == 2
        for part in range(0, heads, 4):
            y = nn(h_all[r, :], w3[j, :, part * HEAD_DIM:(part + 4) * HEAD_DIM])
            c = jnp.where(is_v, 1.0, cos_s[r, :])
            s = jnp.where(is_v, 0.0, sin_s[r, :])
            for n in range(4):
                yn = y[:, n * HEAD_DIM:(n + 1) * HEAD_DIM]
                qkv[j, part + n, r, :] = (yn * c + swap_pairs(yn) * s).astype(BF16)

    h_copy = pltpu.make_async_copy(h_all, h_out, lsem.at[0])
    h_copy.start()

    outs = (ot_out, gq_out, gk_out, gv_out)

    def slab(a, n):
        span = pl.ds(pl.multiple_of(core * width + n * HEAD_DIM, HEAD_DIM), HEAD_DIM)
        return (ot_s.at[n], outs[0].at[span, :]) if a == 0 else (res.at[a - 1, n], outs[a].at[:, span])

    def send_head(a, n):
        src, dst = slab(a, n)
        pltpu.make_async_copy(src, dst, osem.at[a]).start()
        pltpu.make_async_remote_copy(
            src_ref=src, dst_ref=dst, send_sem=xsem.at[0, a], recv_sem=xsem.at[1, a],
            device_id={"sp": partner}, device_id_type=MESH).start()

    def in_turn(streams):
        while streams:
            for g in list(streams):
                if next(g, None) is None:
                    streams.remove(g)

    c2 = SCALE * LOG2E
    causal = (lax.broadcasted_iota(jnp.int32, (QB, QB), 0)
              <= lax.broadcasted_iota(jnp.int32, (QB, QB), 1))

    def tile(i):
        return slice(i * QB, (i + 1) * QB)

    def scores(n, i, j):
        s = nt(qkv[1, n, tile(j), :], qkv[0, n, tile(i), :])
        return jnp.where(causal, s, -jnp.inf) if i == j else s

    def forward(n, slot):
        vt = vt_s.at[slot]
        vt[...] = qkv[2, n].T
        for i in range(nq):
            ss = [scores(n, i, j) for j in range(i + 1)]
            yield True
            m = functools.reduce(jnp.maximum, [jnp.max(s, axis=0, keepdims=True) for s in ss])
            es = [jnp.exp2((s - m) * c2) for s in ss]
            li = 1.0 / sum(jnp.sum(e, axis=0, keepdims=True) for e in es)
            m_s[n, :, tile(i)] = m
            li_s[n, :, tile(i)] = li
            ps = [(e * li).astype(BF16) for e in es]
            yield True
            ot_s[n, :, tile(i)] = sum(nn(vt[:, tile(j)], p) for j, p in enumerate(ps)).astype(BF16)
            yield True

    @pl.loop(0, heads // 2)
    def _(t):
        @pl.when(t == 1)
        def _():
            got(1, 0)
            pass_first(1)

        in_turn([forward(2 * t, 0), forward(2 * t + 1, 1)])
        send_head(0, 2 * t)
        send_head(0, 2 * t + 1)

    @pl.loop(0, n_chips)
    def _(i):
        @pl.when(i == 1)
        def _():
            pass_second(1)
            from_partner(1, (7, 8, 9, 10))

        @pl.when(i == 3)
        def _():
            pass_far(1)
            from_partner(1, (11, 12))

        r = chip_rows(i)
        for part in range(0, heads, 4):
            y = nn(g_all[r, :], wot_s[:, part * HEAD_DIM:(part + 4) * HEAD_DIM])
            for n in range(4):
                do_s[part + n, r, :] = y[:, n * HEAD_DIM:(n + 1) * HEAD_DIM].astype(BF16)

    g_copy = pltpu.make_async_copy(g_all, g_out, lsem.at[1])
    g_copy.start()

    here = pl.ds(pl.multiple_of(chip * rows_chip, rows_chip), rows_chip)
    mine = pl.ds(pl.multiple_of(core * blk, blk), blk)
    theirs = pl.ds(pl.multiple_of(other * blk, blk), blk)

    def swap_part(src, recv, k):
        return pltpu.make_async_remote_copy(
            src_ref=src, dst_ref=recv, send_sem=fsem.at[0, k], recv_sem=fsem.at[1, k],
            device_id={"sp": partner}, device_id_type=MESH)

    o_here = jnp.concatenate([ot_s[n, :, here] for n in range(heads)], axis=0).T
    for n in range(0, model, NT):
        a_part[:, n:n + NT] = nn(o_here, wo_s[:, n:n + NT])
    a_swap = swap_part(a_part.at[theirs, :], a_recv, 0)
    a_swap.start()

    def at(j, i):
        return i * (i + 1) // 2 + j

    def backward(n, slot):
        kt, pt, dst = kt_s.at[slot], pt_s.at[slot], dst_s.at[slot]
        kt[...] = qkv[1, n].T
        for i in reversed(range(nq)):
            q_i, do_i = qkv[0, n, tile(i), :], do_s[n, tile(i), :]
            ss = [scores(n, i, j) for j in range(i + 1)]
            dps = [nt(qkv[2, n, tile(j), :], do_i) for j in range(i + 1)]
            yield True
            m, li = m_s[n, :, tile(i)], li_s[n, :, tile(i)]
            ps = [jnp.exp2((s - m) * c2) * li for s in ss]
            rdot = sum(jnp.sum(p * dp, axis=0, keepdims=True) for p, dp in zip(ps, dps))
            for j in range(i + 1):
                pt[at(j, i)] = ps[j].astype(BF16)
                dst[at(j, i)] = (ps[j] * (dps[j] - rdot) * SCALE).astype(BF16)
            yield True
            dq = sum(nn(kt[:, tile(j)], dst[at(j, i)]) for j in range(i + 1)).T.astype(BF16).astype(F32)
            c, s = cos_s[tile(i), :], sin_s[tile(i), :]
            res[0, n, tile(i), :] = (dq * c - swap_pairs(dq) * s).astype(BF16)
            dk = sum(nn(dst[at(i, k)], qkv[0, n, tile(k), :]) for k in range(i, nq)).astype(BF16).astype(F32)
            res[1, n, tile(i), :] = (dk * c - swap_pairs(dk) * s).astype(BF16)
            res[2, n, tile(i), :] = sum(nn(pt[at(i, k)], do_s[n, tile(k), :]) for k in range(i, nq)).astype(BF16)
            yield True

    @pl.loop(0, heads // 2)
    def _(t):
        in_turn([backward(2 * t, 0), backward(2 * t + 1, 1)])
        for a in (1, 2, 3):
            send_head(a, 2 * t)
            send_head(a, 2 * t + 1)

    def cols_of(j):
        return jnp.concatenate([res[j, n, here, :] for n in range(heads)], axis=1).T

    for j in range(3):
        cols_s[j] = cols_of(j)

    @pl.loop(0, model // MT)
    def _(d):
        r = pl.ds(pl.multiple_of(d * MT, MT), MT)
        dh_t = sum(nn(w3[j, r, :], cols_s[j]) for j in range(3))
        for k in range(CORES):
            dh_part[k, r, :] = dh_t[:, k * blk:(k + 1) * blk]

    dh_swap = swap_part(dh_part.at[other], dh_recv, 1)
    dh_swap.start()
    a_swap.wait()
    a_out[...] = (a_part[mine, :] + a_recv[...]).astype(BF16)
    xhat, rstd = normalize(x_ref[...])
    dh_swap.wait()
    dh = (dh_part[core] + dh_recv[...]).T
    dl_buf[me] = jnp.sum(dh * xhat, axis=0, keepdims=True)
    small_send(dl_buf, dsem)
    dy = dh * ln_w
    dx = dy - jnp.mean(dy, axis=-1, keepdims=True) - xhat * jnp.mean(dy * xhat, axis=-1, keepdims=True)
    dx_out[...] = (dx * rstd).astype(BF16)

    h_copy.wait()
    g_copy.wait()
    for a in range(2):
        for kind, (block, piece, to) in sends.items():
            copy(a, kind, block, piece, to).wait_send()
    my_span = pl.ds(pl.multiple_of(core * width, width), width)
    their_span = pl.ds(pl.multiple_of(other * width, width), width)
    for a in range(4):
        sent = outs[a].at[my_span, :] if a == 0 else outs[a].at[:, my_span]
        came = outs[a].at[their_span, :] if a == 0 else outs[a].at[:, their_span]
        pltpu.make_async_copy(sent, sent, osem.at[a]).wait()
        done = pltpu.make_async_remote_copy(
            src_ref=sent, dst_ref=came, send_sem=xsem.at[0, a], recv_sem=xsem.at[1, a],
            device_id={"sp": partner}, device_id_type=MESH)
        done.wait_send()
        done.wait_recv()
    small_wait(dl_buf, dsem)
    total = dl_buf[0]
    for k in range(1, n_dev):
        total = total + dl_buf[k]
    dl_out[...] = total.astype(BF16).reshape(model)


def run_main(n_dev, hidden, d_attn, positions, ln_weight, w_q, w_k, w_v, w_o):
    blk, model = hidden.shape
    seq = n_dev * blk
    width = w_q.shape[1] // CORES
    heads = width // HEAD_DIM
    pairs = (seq // QB) * (seq // QB + 1) // 2
    vm = pl.BlockSpec(memory_space=pltpu.VMEM)
    hbm = pl.BlockSpec(memory_space=pl.ANY)
    full = jax.ShapeDtypeStruct((seq, model), BF16)
    wide = jax.ShapeDtypeStruct((seq, w_q.shape[1]), BF16)
    rows = jax.ShapeDtypeStruct((blk, model), BF16)
    freq = jnp.repeat(ROPE_BASE ** (-jnp.arange(0, HEAD_DIM, 2, dtype=F32) / HEAD_DIM), 2)[None, :]
    return pl.pallas_call(
        functools.partial(main_kernel, n_dev),
        out_shape=(full, full, jax.ShapeDtypeStruct((w_q.shape[1], seq), BF16), wide, wide, wide, rows, rows, jax.ShapeDtypeStruct((model,), BF16)),
        in_specs=[vm] * 5 + [hbm] * 4,
        out_specs=[hbm] * 6 + [vm] * 3,
        scratch_shapes=[
            pltpu.VMEM((seq, model), BF16),
            pltpu.VMEM((seq, model), BF16),
            pltpu.VMEM((n_dev, 1, blk), jnp.int32),
            pltpu.VMEM((seq, HEAD_DIM), F32),
            pltpu.VMEM((seq, HEAD_DIM), F32),
            pltpu.VMEM((3, model, width), BF16),
            pltpu.VMEM((width, model), BF16),
            pltpu.VMEM((model, width), BF16),
            pltpu.VMEM((3, heads, seq, HEAD_DIM), BF16),
            pltpu.VMEM((heads, seq, HEAD_DIM), BF16),
            pltpu.VMEM((heads, HEAD_DIM, seq), BF16),
            pltpu.VMEM((3, heads, seq, HEAD_DIM), BF16),
            pltpu.VMEM((heads, 1, seq), F32),
            pltpu.VMEM((heads, 1, seq), F32),
            pltpu.VMEM((2, HEAD_DIM, seq), BF16),
            pltpu.VMEM((2, HEAD_DIM, seq), BF16),
            pltpu.VMEM((2, pairs, QB, QB), BF16),
            pltpu.VMEM((2, pairs, QB, QB), BF16),
            pltpu.VMEM((CORES * blk, model), F32),
            pltpu.VMEM((blk, model), F32),
            pltpu.VMEM((CORES, model, blk), F32),
            pltpu.VMEM((model, blk), F32),
            pltpu.VMEM((3, width, CORES * blk), BF16),
            pltpu.VMEM((n_dev, 1, model), F32),
            pltpu.SemaphoreType.DMA((2, 13)),
            pltpu.SemaphoreType.DMA((2, 13)),
            pltpu.SemaphoreType.DMA((4,)),
            pltpu.SemaphoreType.DMA((2,)),
            pltpu.SemaphoreType.DMA((2, 4)),
            pltpu.SemaphoreType.DMA((4,)),
            pltpu.SemaphoreType.DMA((2, n_dev)),
            pltpu.SemaphoreType.DMA((2, n_dev)),
            pltpu.SemaphoreType.DMA((2, 2)),
        ],
        compiler_params=pltpu.CompilerParams(
            collective_id=0, has_side_effects=True, vmem_limit_bytes=VMEM_LIMIT),
        name="gather_attention",
    )(hidden, d_attn, positions, freq, ln_weight, w_q, w_k, w_v, w_o)


def grad_kernel(ot, g, h, gq, gk, gv, a_in, dx_in, dl_in, dq_out, dk_out, dv_out, do_out, a_out, dx_out, dl_out,
                ot_v, g_v, h_v, ht_v, g3, out_v, a_v, dx_v, sem, msem, usem):
    tiles = ot.shape[0] // MT
    wide = g.shape[1]
    outs = (dq_out, dk_out, dv_out)

    def rows(m):
        return pl.ds(pl.multiple_of(m * MT, MT), MT)

    ot_loads = [pltpu.make_async_copy(ot.at[rows(m), :], ot_v.at[rows(m), :], msem.at[m]) for m in range(tiles)]
    g_load = pltpu.make_async_copy(g, g_v, sem.at[0])
    h_load = pltpu.make_async_copy(h, h_v, sem.at[1])
    g3_loads = [pltpu.make_async_copy(x, g3.at[k], sem.at[2 + k]) for k, x in enumerate((gq, gk, gv))]
    small_in = [pltpu.make_async_copy(a_in, a_v, sem.at[5]), pltpu.make_async_copy(dx_in, dx_v, sem.at[6])]
    small_out = [pltpu.make_async_copy(a_v, a_out, sem.at[5]), pltpu.make_async_copy(dx_v, dx_out, sem.at[6])]
    ot_loads[0].start()
    g_load.start()
    h_load.start()
    for c in ot_loads[1:] + g3_loads + small_in:
        c.start()
    dl_out[...] = dl_in[...]

    def store(slot, out, m):
        return pltpu.make_async_copy(out_v.at[slot], out.at[rows(m), :], usem.at[slot])

    def product(slot, a, b):
        for n in range(0, wide, NT):
            out_v[slot, :, n:n + NT] = nn(a, b[:, n:n + NT]).astype(BF16)

    def turn(m):
        ht_v[rows(m), :] = h_v[:, rows(m)].T

    for m in range(tiles):
        ot_loads[m].wait()
        if m == 0:
            g_load.wait()
        if m == 1:
            h_load.wait()
        if m >= 2:
            store(m % 2, do_out, m - 2).wait()
        if m >= 1:
            turn(m - 1)
        product(m % 2, ot_v[m * MT:(m + 1) * MT, :], g_v)
        store(m % 2, do_out, m).start()

    turn(tiles - 1)
    for c in small_in:
        c.wait()
    for c in small_out:
        c.start()

    @pl.loop(0, 3 * tiles)
    def _(it):
        k, m, slot = it // tiles, lax.rem(it, tiles), lax.rem(it, 2)
        for j in range(3):
            @pl.when(it == j * tiles)
            def _():
                g3_loads[j].wait()

        store(slot, do_out, 0).wait()
        product(slot, ht_v[rows(m), :], g3.at[k])
        for j in range(3):
            @pl.when(k == j)
            def _():
                store(slot, outs[j], m).start()

    for slot in range(2):
        store(slot, do_out, 0).wait()
    for c in small_out:
        c.wait()


def run_grads(h, g, ot, gq, gk, gv, attn_out, d_hid, d_lnw):
    seq, model = h.shape
    wide = gq.shape[1]
    tiles = model // MT
    hbm = pl.BlockSpec(memory_space=pl.ANY)
    vm = pl.BlockSpec(memory_space=pltpu.VMEM)
    grad = jax.ShapeDtypeStruct((model, wide), BF16)

    def like(a):
        return jax.ShapeDtypeStruct(a.shape, a.dtype)

    return pl.pallas_call(
        grad_kernel,
        out_shape=[grad, grad, grad, jax.ShapeDtypeStruct((wide, model), BF16),
                   like(attn_out), like(d_hid), like(d_lnw)],
        in_specs=[hbm] * 8 + [vm],
        out_specs=[hbm] * 6 + [vm],
        scratch_shapes=[
            pltpu.VMEM((wide, seq), BF16),
            pltpu.VMEM((seq, model), BF16),
            pltpu.VMEM((seq, model), BF16),
            pltpu.VMEM((model, seq), BF16),
            pltpu.VMEM((3, seq, wide), BF16),
            pltpu.VMEM((2, MT, wide), BF16),
            pltpu.VMEM(attn_out.shape, BF16),
            pltpu.VMEM(d_hid.shape, BF16),
            pltpu.SemaphoreType.DMA((7,)),
            pltpu.SemaphoreType.DMA((tiles,)),
            pltpu.SemaphoreType.DMA((2,)),
        ],
        compiler_params=pltpu.CompilerParams(vmem_limit_bytes=VMEM_LIMIT),
        name="weight_grads",
    )(ot, g, h, gq, gk, gv, attn_out, d_hid, d_lnw)


def solution(mesh):
    n_dev = mesh.shape['sp']
    row_spec = P(('dp', 'sp'), None)
    full_spec = P(None, None)
    grad_spec = P('dp', None)

    def local_step(hidden, positions, d_attn, ln_weight, w_q, w_k, w_v, w_o):
        h, g, ot, gq, gk, gv, attn_out, d_hid, d_lnw = run_main(
            n_dev, hidden, d_attn, positions, ln_weight, w_q, w_k, w_v, w_o)
        dwq, dwk, dwv, dwo, attn_out, d_hid, d_lnw = run_grads(h, g, ot, gq, gk, gv, attn_out, d_hid, d_lnw)
        return attn_out, d_hid, d_lnw, dwq, dwk, dwv, dwo

    return jax.shard_map(local_step, mesh=mesh,
                         in_specs=(row_spec, P(('dp', 'sp')), row_spec, P(None), full_spec, full_spec, full_spec, full_spec),
                         out_specs=(row_spec, row_spec, P('dp'), grad_spec, grad_spec, grad_spec, grad_spec),
                         check_vma=False)
```

```python
import functools

import jax
import jax.numpy as jnp
from jax import lax
from jax.experimental import pallas as pl
from jax.experimental.pallas import tpu as pltpu
from jax.sharding import PartitionSpec as P

HEAD_DIM = 128
LN_EPS = 1e-5
ROPE_BASE = 10000.0
SCALE = HEAD_DIM ** -0.5
LOG2E = 1.4426950408889634
CORES = 2
QB = 256
MT = 512
NT = 1024
VMEM_LIMIT = 67043328
MESH = pl.DeviceIdType.MESH
F32 = jnp.float32
BF16 = jnp.bfloat16


def normalize(x):
    x = x.astype(F32)
    centered = x - jnp.mean(x, axis=-1, keepdims=True)
    rstd = lax.rsqrt(jnp.mean(centered * centered, axis=-1, keepdims=True) + LN_EPS)
    return centered * rstd, rstd


def sin_cos(a):
    n = jnp.floor(a * 0.6366197723675814 + 0.5)
    r = ((a - n * 1.5703125) - n * 4.8375129699707031e-4) - n * 7.5497899548918821e-8
    z = r * r
    s = r + r * z * (-1.6666654611e-1 + z * (8.3321608736e-3 + z * -1.9515295891e-4))
    c = 1.0 - 0.5 * z + z * z * (4.166664568298827e-2 + z * (-1.388731625493765e-3 + z * 2.443315711809948e-5))
    quad = n.astype(jnp.int32)
    odd = (quad & 1) == 1
    sin = jnp.where(odd, c, s)
    cos = jnp.where(odd, s, c)
    return jnp.where((quad & 2) == 2, -sin, sin), jnp.where(((quad + 1) & 2) == 2, -cos, cos)


def even_lanes(shape):
    return lax.broadcasted_iota(jnp.int32, shape, 1) % 2 == 0


def swap_pairs(y):
    return jnp.where(even_lanes(y.shape), pltpu.roll(y, HEAD_DIM - 1, 1), pltpu.roll(y, 1, 1))


def nt(a, b):
    return lax.dot_general(a, b, (((1,), (1,)), ((), ())), preferred_element_type=F32)


def nn(a, b):
    return jnp.dot(a, b, preferred_element_type=F32)


def main_kernel(n_dev, x_ref, g_ref, p_ref, f_ref, w_ref, wq, wk, wv, wo,
                ht_out, dwo_out, gq_out, gk_out, dwv_out, a_out, dx_out, dl_out,
                h_all, g_all, pos, cos_s, sin_s, w3, wo_s, wot_s, qkv, do_s,
                ot_s, res, m_s, li_s, kt_s, vt_s, pt_s, dst_s, a_part, a_recv, dh_part, dh_recv, cols_s, dl_buf,
                ssem, rsem, wsem, lsem, xsem, osem, psem, dsem, fsem):
    blk, model = x_ref.shape
    half = blk // 2
    rows_chip = CORES * blk
    n_chips = n_dev // CORES
    heads = qkv.shape[1]
    width = heads * HEAD_DIM
    seq = n_dev * blk
    nq = seq // QB

    me = lax.axis_index("sp")
    chip, core = me // CORES, lax.rem(me, CORES)
    other = 1 - core

    def dev(step, cr):
        return lax.rem(chip + step + n_chips, n_chips) * CORES + cr

    partner, right, left = dev(0, other), dev(1, core), dev(-1, core)
    others = [lax.rem(me + k, n_dev) for k in range(1, n_dev)]

    barrier = pltpu.get_barrier_semaphore()
    for d in others:
        pl.semaphore_signal(barrier, inc=1, device_id={"sp": d}, device_id_type=MESH)

    col0 = pl.multiple_of(core * width, width)
    wcopies = [
        pltpu.make_async_copy(w.at[:, pl.ds(col0, width)], w3.at[j], wsem.at[j])
        for j, w in enumerate((wq, wk, wv))
    ]
    wcopies.append(pltpu.make_async_copy(wo.at[pl.ds(col0, width), :], wo_s, wsem.at[3]))
    for c in wcopies:
        c.start()

    own = pl.ds(pl.multiple_of(me * blk, blk), blk)
    ln_w = w_ref[...].astype(F32).reshape(1, model)
    h_all[own, :] = (normalize(x_ref[...])[0] * ln_w).astype(BF16)
    g_all[own, :] = g_ref[...]
    pos[me] = p_ref[...].reshape(1, blk)

    arrays = (h_all, g_all)

    def region(block, piece):
        if piece is None:
            return pl.ds(pl.multiple_of(block * blk, blk), blk)
        return pl.ds(pl.multiple_of(block * blk + piece * half, half), half)

    def copy(a, kind, block, piece, to):
        r = region(block, piece)
        return pltpu.make_async_remote_copy(
            src_ref=arrays[a].at[r, :], dst_ref=arrays[a].at[r, :],
            send_sem=ssem.at[a, kind], recv_sem=rsem.at[a, kind],
            device_id={"sp": to}, device_id_type=MESH)

    far = 2
    sends = {
        0: (me, None, partner),
        1: (me, 0, right), 2: (me, 1, right),
        3: (me, 0, left), 4: (me, 1, left),
        5: (dev(-1, core), 0, right), 6: (dev(1, core), 1, left),
        7: (dev(-1, core), 0, partner), 8: (dev(-1, core), 1, partner),
        9: (dev(1, core), 0, partner), 10: (dev(1, core), 1, partner),
        11: (dev(far, core), 0, partner), 12: (dev(far, core), 1, partner),
    }
    recvs = {
        0: (partner, None),
        1: (dev(-1, core), 0), 2: (dev(-1, core), 1),
        3: (dev(1, core), 0), 4: (dev(1, core), 1),
        5: (dev(far, core), 0), 6: (dev(far, core), 1),
        7: (dev(-1, other), 0), 8: (dev(-1, other), 1),
        9: (dev(1, other), 0), 10: (dev(1, other), 1),
        11: (dev(far, other), 0), 12: (dev(far, other), 1),
    }

    def send(a, kind):
        block, piece, to = sends[kind]
        copy(a, kind, block, piece, to).start()

    def got(a, kind):
        block, piece = recvs[kind]
        copy(a, kind, block, piece, partner).wait_recv()

    def small(buf, sems, k, source, to):
        return pltpu.make_async_remote_copy(
            src_ref=buf.at[source], dst_ref=buf.at[source],
            send_sem=sems.at[0, k], recv_sem=sems.at[1, k],
            device_id={"sp": to}, device_id_type=MESH)

    def small_send(buf, sems):
        for k in range(1, n_dev):
            small(buf, sems, k, me, others[k - 1]).start()

    def small_wait(buf, sems):
        for k in range(1, n_dev):
            small(buf, sems, k, lax.rem(me - k + n_dev, n_dev), partner).wait_recv()
        for k in range(1, n_dev):
            small(buf, sems, k, me, partner).wait_send()

    pl.semaphore_wait(barrier, n_dev - 1)
    small_send(pos, psem)
    for kind in (1, 4, 2, 3, 0):
        send(0, kind)
    send(1, 0)

    def pass_first(a):
        got(a, 1)
        send(a, 5)
        send(a, 7)
        got(a, 4)
        send(a, 6)
        send(a, 10)

    def pass_second(a):
        got(a, 2)
        send(a, 8)
        got(a, 3)
        send(a, 9)

    def pass_far(a):
        got(a, 5)
        send(a, 11)
        got(a, 6)
        send(a, 12)

    def from_partner(a, which):
        for kind in which:
            got(a, kind)

    def chip_rows(i):
        step = lax.rem(i * (i + 1) // 2, n_chips)
        return pl.ds(pl.multiple_of(lax.rem(chip + step, n_chips) * rows_chip, rows_chip), rows_chip)

    def fill_tables():
        small_wait(pos, psem)
        diag = (lax.broadcasted_iota(jnp.int32, (blk, blk), 0)
                == lax.broadcasted_iota(jnp.int32, (blk, blk), 1))
        even = even_lanes((blk, HEAD_DIM))

        @pl.loop(0, n_dev)
        def _(b):
            r = pl.ds(pl.multiple_of(b * blk, blk), blk)
            p = jnp.broadcast_to(pos[b].astype(F32), (blk, blk))
            col = jnp.sum(jnp.where(diag, p, 0.0), axis=1, keepdims=True)
            sin, cos = sin_cos(col * f_ref[...])
            cos_s[r, :] = cos
            sin_s[r, :] = jnp.where(even, -sin, sin)

    def project_do(r):
        for part in range(0, heads, 4):
            y = nn(g_all[r, :], wot_s[:, part * HEAD_DIM:(part + 4) * HEAD_DIM])
            for n in range(4):
                do_s[part + n, r, :] = y[:, n * HEAD_DIM:(n + 1) * HEAD_DIM].astype(BF16)

    def job_rows(i):
        mid, late = (lax.rem(i, 3) + 1) // 2, i // 2
        runs = []
        for k in range(4):
            beside = (n_chips - 1, half * late + blk * k) if k < 2 else (1, half * (1 - late) + blk * (k - 2))
            step = (1 - mid) * (i // 3) * far + mid * beside[0]
            row = lax.rem(chip + step, n_chips) * rows_chip + (1 - mid) * half * k + mid * beside[1]
            runs.append(pl.ds(pl.multiple_of(row, half), half))
        return runs

    @pl.loop(0, n_chips)
    def _(i):
        @pl.when(i == 0)
        def _():
            fill_tables()
            got(0, 0)
            for c in wcopies:
                c.wait()

        @pl.when(i == 1)
        def _():
            for e in range(width // QB):
                wot_s[:, e * QB:(e + 1) * QB] = wo_s[e * QB:(e + 1) * QB, :].T
            got(1, 0)
            project_do(chip_rows(0))
            pass_first(0)
            for kind in (1, 4, 2, 3):
                send(1, kind)
            from_partner(0, (7, 10))

        @pl.when(i == 2)
        def _():
            pass_second(0)
            from_partner(0, (8, 9))

        @pl.when(i == 3)
        def _():
            pass_far(0)
            from_partner(0, (11, 12))

        runs = job_rows(i)

        def rows_of(ref):
            return jnp.concatenate([ref[r, :] for r in runs], axis=0)

        x = rows_of(h_all)
        c, s = rows_of(cos_s), rows_of(sin_s)
        for j in range(3):
            for part in range(0, heads, 4):
                y = nn(x, w3[j, :, part * HEAD_DIM:(part + 4) * HEAD_DIM])
                for n in range(4):
                    yn = y[:, n * HEAD_DIM:(n + 1) * HEAD_DIM]
                    yn = (yn if j == 2 else yn * c + swap_pairs(yn) * s).astype(BF16)
                    for k, r in enumerate(runs):
                        qkv[j, part + n, r, :] = yn[k * half:(k + 1) * half]


    outs = (dwo_out, gq_out, gk_out, dwv_out)
    my_col = core * width

    def give(a, src, dst):
        pltpu.make_async_copy(src, dst, osem.at[a]).start()
        pltpu.make_async_remote_copy(
            src_ref=src, dst_ref=dst, send_sem=xsem.at[0, a], recv_sem=xsem.at[1, a],
            device_id={"sp": partner}, device_id_type=MESH).start()

    def head_cols(n):
        return pl.ds(pl.multiple_of(my_col + n * HEAD_DIM, HEAD_DIM), HEAD_DIM)

    def rows_tile(m):
        return pl.ds(pl.multiple_of(m * MT, MT), MT)

    def in_turn(streams):
        while streams:
            for g in list(streams):
                if next(g, None) is None:
                    streams.remove(g)

    c2 = SCALE * LOG2E
    causal = (lax.broadcasted_iota(jnp.int32, (QB, QB), 0)
              <= lax.broadcasted_iota(jnp.int32, (QB, QB), 1))

    def tile(i):
        return slice(i * QB, (i + 1) * QB)

    def scores(n, i, j):
        s = nt(qkv[1, n, tile(j), :], qkv[0, n, tile(i), :])
        return jnp.where(causal, s, -jnp.inf) if i == j else s

    def forward(n, slot):
        vt = vt_s.at[slot]
        vt[...] = qkv[2, n].T
        for i in range(nq):
            ss = [scores(n, i, j) for j in range(i + 1)]
            yield True
            m = functools.reduce(jnp.maximum, [jnp.max(s, axis=0, keepdims=True) for s in ss])
            es = [jnp.exp2((s - m) * c2) for s in ss]
            li = 1.0 / sum(jnp.sum(e, axis=0, keepdims=True) for e in es)
            m_s[n, :, tile(i)] = m
            li_s[n, :, tile(i)] = li
            ps = [(e * li).astype(BF16) for e in es]
            yield True
            ot_s[n, :, tile(i)] = sum(nn(vt[:, tile(j)], p) for j, p in enumerate(ps)).astype(BF16)
            yield True

    @pl.loop(0, heads // 2)
    def _(t):
        @pl.when(t == 1)
        def _():
            pass_first(1)

        in_turn([forward(2 * t, 0), forward(2 * t + 1, 1)])

    here = pl.ds(pl.multiple_of(chip * rows_chip, rows_chip), rows_chip)
    mine = pl.ds(pl.multiple_of(core * blk, blk), blk)
    theirs = pl.ds(pl.multiple_of(other * blk, blk), blk)

    def swap_part(src, recv, k):
        return pltpu.make_async_remote_copy(
            src_ref=src, dst_ref=recv, send_sem=fsem.at[0, k], recv_sem=fsem.at[1, k],
            device_id={"sp": partner}, device_id_type=MESH)

    a_swap = swap_part(a_part.at[theirs, :], a_recv, 0)

    @pl.loop(1, n_chips)
    def _(i):
        @pl.when(i == 1)
        def _():
            pass_second(1)
            from_partner(1, (7, 8, 9, 10))

        @pl.when(i == 3)
        def _():
            o_here = jnp.concatenate([ot_s[n, :, here] for n in range(heads)], axis=0).T
            for n in range(0, model, NT):
                a_part[:, n:n + NT] = nn(o_here, wo_s[:, n:n + NT])
            a_swap.start()
            pass_far(1)
            from_partner(1, (11, 12))

        project_do(chip_rows(i))

    for kind, (block, piece, to) in sends.items():
        copy(0, kind, block, piece, to).wait_send()
    for e in range(0, model, QB):
        wot_s[e:e + QB, :] = h_all[:, e:e + QB].T
    ht_copy = pltpu.make_async_copy(wot_s, ht_out, lsem.at[0])
    ht_copy.start()

    @pl.loop(0, width // MT)
    def _(m):
        per = MT // HEAD_DIM
        o_t = jnp.concatenate([ot_s[m * per + n] for n in range(per)], axis=0)
        for n in range(0, model, NT):
            h_all[rows_tile(m), n:n + NT] = nn(o_t, g_all[:, n:n + NT]).astype(BF16)
        give(0, h_all.at[rows_tile(m), :], dwo_out.at[pl.ds(pl.multiple_of(my_col + m * MT, MT), MT), :])

    def at(j, i):
        return i * (i + 1) // 2 + j

    def backward(n, slot):
        kt, pt, dst = kt_s.at[slot], pt_s.at[slot], dst_s.at[slot]
        kt[...] = qkv[1, n].T
        for i in reversed(range(nq)):
            q_i, do_i = qkv[0, n, tile(i), :], do_s[n, tile(i), :]
            m, li = m_s[n, :, tile(i)], li_s[n, :, tile(i)]
            ps, ts, rdot = [], [], 0.0
            s, dp = scores(n, i, 0), nt(qkv[2, n, tile(0), :], do_i)
            for j in range(i + 1):
                yield True
                p = jnp.exp2((s - m) * c2) * li
                t = p * dp
                rdot = rdot + jnp.sum(t, axis=0, keepdims=True)
                pt[at(j, i)] = p.astype(BF16)
                ps.append(p)
                ts.append(t)
                if j < i:
                    s, dp = scores(n, i, j + 1), nt(qkv[2, n, tile(j + 1), :], do_i)
            yield True
            for j in range(i + 1):
                dst[at(j, i)] = ((ts[j] - ps[j] * rdot) * SCALE).astype(BF16)
            yield True
            dq = sum(nn(kt[:, tile(j)], dst[at(j, i)]) for j in range(i + 1)).T.astype(BF16).astype(F32)
            c, s = cos_s[tile(i), :], sin_s[tile(i), :]
            res[0, n, tile(i), :] = (dq * c - swap_pairs(dq) * s).astype(BF16)
            dk = sum(nn(dst[at(i, k)], qkv[0, n, tile(k), :]) for k in range(i, nq)).astype(BF16).astype(F32)
            res[1, n, tile(i), :] = (dk * c - swap_pairs(dk) * s).astype(BF16)
            res[2, n, tile(i), :] = sum(nn(pt[at(i, k)], do_s[n, tile(k), :]) for k in range(i, nq)).astype(BF16)
            yield True

    @pl.loop(0, heads // 2)
    def _(t):
        in_turn([backward(2 * t, 0), backward(2 * t + 1, 1)])
        for a in (1, 2):
            for n in (2 * t, 2 * t + 1):
                give(a, res.at[a - 1, n], outs[a].at[:, head_cols(n)])

    def cols_of(j):
        return jnp.concatenate([res[j, n, here, :] for n in range(heads)], axis=1).T

    for j in range(3):
        cols_s[j] = cols_of(j)

    @pl.loop(0, model // MT)
    def _(d):
        r = pl.ds(pl.multiple_of(d * MT, MT), MT)
        dh_t = sum(nn(w3[j, r, :], cols_s[j]) for j in range(3))
        for k in range(CORES):
            dh_part[k, r, :] = dh_t[:, k * blk:(k + 1) * blk]

    dh_swap = swap_part(dh_part.at[other], dh_recv, 1)
    dh_swap.start()

    def finish_rows():
        a_swap.wait()
        a_out[...] = (a_part[mine, :] + a_recv[...]).astype(BF16)
        xhat, rstd = normalize(x_ref[...])
        dh_swap.wait()
        dh = (dh_part[core] + dh_recv[...]).T
        dl_buf[me] = jnp.sum(dh * xhat, axis=0, keepdims=True)
        small_send(dl_buf, dsem)
        dy = dh * ln_w
        dx = dy - jnp.mean(dy, axis=-1, keepdims=True) - xhat * jnp.mean(dy * xhat, axis=-1, keepdims=True)
        dx_out[...] = (dx * rstd).astype(BF16)

    @pl.loop(0, model // MT)
    def _(m):
        @pl.when(m == 2)
        def _():
            finish_rows()

        per = seq // MT
        place = pl.ds(pl.multiple_of(lax.rem(m, per) * MT, MT), MT)
        for part in range(0, heads, 4):
            gv = jnp.concatenate([res[2, part + n] for n in range(4)], axis=1)
            y = nn(wot_s[rows_tile(m), :], gv).astype(BF16)
            for n in range(4):
                qkv[m // per, part + n, place, :] = y[:, n * HEAD_DIM:(n + 1) * HEAD_DIM]
        for n in range(heads):
            give(3, qkv.at[m // per, n, place, :], dwv_out.at[rows_tile(m), head_cols(n)])

    ht_copy.wait()
    for kind, (block, piece, to) in sends.items():
        copy(1, kind, block, piece, to).wait_send()
    my_span = pl.ds(pl.multiple_of(core * width, width), width)
    their_span = pl.ds(pl.multiple_of(other * width, width), width)
    for a in range(4):
        sent = outs[a].at[my_span, :] if a == 0 else outs[a].at[:, my_span]
        came = outs[a].at[their_span, :] if a == 0 else outs[a].at[:, their_span]
        pltpu.make_async_copy(sent, sent, osem.at[a]).wait()
        done = pltpu.make_async_remote_copy(
            src_ref=sent, dst_ref=came, send_sem=xsem.at[0, a], recv_sem=xsem.at[1, a],
            device_id={"sp": partner}, device_id_type=MESH)
        done.wait_send()
        done.wait_recv()
    small_wait(dl_buf, dsem)
    total = dl_buf[0]
    for k in range(1, n_dev):
        total = total + dl_buf[k]
    dl_out[...] = total.astype(BF16).reshape(model)


def run_main(n_dev, hidden, d_attn, positions, ln_weight, w_q, w_k, w_v, w_o):
    blk, model = hidden.shape
    seq = n_dev * blk
    width = w_q.shape[1] // CORES
    heads = width // HEAD_DIM
    pairs = (seq // QB) * (seq // QB + 1) // 2
    vm = pl.BlockSpec(memory_space=pltpu.VMEM)
    hbm = pl.BlockSpec(memory_space=pl.ANY)
    full = w_q.shape[1]
    wide = jax.ShapeDtypeStruct((seq, full), BF16)
    rows = jax.ShapeDtypeStruct((blk, model), BF16)
    freq = jnp.repeat(ROPE_BASE ** (-jnp.arange(0, HEAD_DIM, 2, dtype=F32) / HEAD_DIM), 2)[None, :]
    return pl.pallas_call(
        functools.partial(main_kernel, n_dev),
        out_shape=(jax.ShapeDtypeStruct((model, seq), BF16), jax.ShapeDtypeStruct((full, model), BF16),
                   wide, wide, jax.ShapeDtypeStruct((model, full), BF16), rows, rows, jax.ShapeDtypeStruct((model,), BF16)),
        in_specs=[vm] * 5 + [hbm] * 4,
        out_specs=[hbm] * 5 + [vm] * 3,
        scratch_shapes=[
            pltpu.VMEM((seq, model), BF16),
            pltpu.VMEM((seq, model), BF16),
            pltpu.VMEM((n_dev, 1, blk), jnp.int32),
            pltpu.VMEM((seq, HEAD_DIM), F32),
            pltpu.VMEM((seq, HEAD_DIM), F32),
            pltpu.VMEM((3, model, width), BF16),
            pltpu.VMEM((width, model), BF16),
            pltpu.VMEM((model, width), BF16),
            pltpu.VMEM((3, heads, seq, HEAD_DIM), BF16),
            pltpu.VMEM((heads, seq, HEAD_DIM), BF16),
            pltpu.VMEM((heads, HEAD_DIM, seq), BF16),
            pltpu.VMEM((3, heads, seq, HEAD_DIM), BF16),
            pltpu.VMEM((heads, 1, seq), F32),
            pltpu.VMEM((heads, 1, seq), F32),
            pltpu.VMEM((2, HEAD_DIM, seq), BF16),
            pltpu.VMEM((2, HEAD_DIM, seq), BF16),
            pltpu.VMEM((2, pairs, QB, QB), BF16),
            pltpu.VMEM((2, pairs, QB, QB), BF16),
            pltpu.VMEM((CORES * blk, model), F32),
            pltpu.VMEM((blk, model), F32),
            pltpu.VMEM((CORES, model, blk), F32),
            pltpu.VMEM((model, blk), F32),
            pltpu.VMEM((3, width, CORES * blk), BF16),
            pltpu.VMEM((n_dev, 1, model), F32),
            pltpu.SemaphoreType.DMA((2, 13)),
            pltpu.SemaphoreType.DMA((2, 13)),
            pltpu.SemaphoreType.DMA((4,)),
            pltpu.SemaphoreType.DMA((1,)),
            pltpu.SemaphoreType.DMA((2, 4)),
            pltpu.SemaphoreType.DMA((4,)),
            pltpu.SemaphoreType.DMA((2, n_dev)),
            pltpu.SemaphoreType.DMA((2, n_dev)),
            pltpu.SemaphoreType.DMA((2, 2)),
        ],
        compiler_params=pltpu.CompilerParams(
            collective_id=0, has_side_effects=True, vmem_limit_bytes=VMEM_LIMIT),
        name="gather_attention",
    )(hidden, d_attn, positions, freq, ln_weight, w_q, w_k, w_v, w_o)


def grad_kernel(ht, gq, gk, dwo_in, dwv_in, a_in, dx_in, dl_in,
                dq_out, dk_out, dwo_out, dwv_out, a_out, dx_out, dl_out,
                ht_v, g2, out_v, dwo_v, dwv_v, a_v, dx_v, hsem, gsem, usem, isem, osem, rsem):
    tiles = ht.shape[0] // MT
    steps = 2 * tiles
    wide = gq.shape[1]
    part = dwo_in.shape[0] // steps
    outs = (dq_out, dk_out)

    def rows(m, size=MT):
        return pl.ds(pl.multiple_of(m * size, size), size)

    ht_loads = [pltpu.make_async_copy(ht.at[rows(m), :], ht_v.at[rows(m), :], hsem.at[m]) for m in range(tiles)]
    g_loads = [pltpu.make_async_copy(x, g2.at[k], gsem.at[k]) for k, x in enumerate((gq, gk))]
    row_in = [pltpu.make_async_copy(a_in, a_v, rsem.at[0]), pltpu.make_async_copy(dx_in, dx_v, rsem.at[1])]
    row_out = [pltpu.make_async_copy(a_v, a_out, rsem.at[0]), pltpu.make_async_copy(dx_v, dx_out, rsem.at[1])]

    def bring(k, it):
        src, buf = ((dwo_in, dwo_v), (dwv_in, dwv_v))[k]
        return pltpu.make_async_copy(src.at[rows(it, part), :], buf.at[rows(it, part), :], isem.at[k, it])

    def put(k, it):
        buf, dst = ((dwo_v, dwo_out), (dwv_v, dwv_out))[k]
        return pltpu.make_async_copy(buf.at[rows(it, part), :], dst.at[rows(it, part), :], osem.at[k, it])

    def store(slot, out, m):
        return pltpu.make_async_copy(out_v.at[slot], out.at[rows(m), :], usem.at[slot])

    ht_loads[0].start()
    g_loads[0].start()
    for c in ht_loads[1:] + g_loads[1:] + row_in:
        c.start()
    for it in range(steps):
        for k in range(2):
            bring(k, it).start()
    dl_out[...] = dl_in[...]

    @pl.loop(0, steps)
    def _(it):
        k, m, slot = it // tiles, lax.rem(it, tiles), lax.rem(it, 2)
        for j in range(tiles):
            @pl.when(it == j)
            def _():
                ht_loads[j].wait()
        for j in range(2):
            @pl.when(it == j * tiles)
            def _():
                g_loads[j].wait()

        @pl.when(it == 1)
        def _():
            for c, d in zip(row_in, row_out):
                c.wait()
                d.start()

        @pl.when(it >= 2)
        def _():
            store(slot, dq_out, 0).wait()

        for n in range(0, wide, NT):
            out_v[slot, :, n:n + NT] = nn(ht_v[rows(m), :], g2[k, :, n:n + NT]).astype(BF16)
        for j in range(2):
            @pl.when(k == j)
            def _():
                store(slot, outs[j], m).start()
            bring(j, it).wait()
            put(j, it).start()

    for slot in range(2):
        store(slot, dq_out, 0).wait()
    for it in range(steps):
        for k in range(2):
            put(k, it).wait()
    for d in row_out:
        d.wait()


def run_grads(ht, dwo, gq, gk, dwv, attn_out, d_hid, d_lnw):
    model, seq = ht.shape
    wide = gq.shape[1]
    tiles = model // MT
    hbm = pl.BlockSpec(memory_space=pl.ANY)
    vm = pl.BlockSpec(memory_space=pltpu.VMEM)

    def like(a):
        return jax.ShapeDtypeStruct(a.shape, a.dtype)

    grad = jax.ShapeDtypeStruct((model, wide), BF16)
    return pl.pallas_call(
        grad_kernel,
        out_shape=[grad, grad, like(dwo), like(dwv), like(attn_out), like(d_hid), like(d_lnw)],
        in_specs=[hbm] * 7 + [vm],
        out_specs=[hbm] * 6 + [vm],
        scratch_shapes=[
            pltpu.VMEM((model, seq), BF16),
            pltpu.VMEM((2, seq, wide), BF16),
            pltpu.VMEM((2, MT, wide), BF16),
            pltpu.VMEM(dwo.shape, BF16),
            pltpu.VMEM(dwv.shape, BF16),
            pltpu.VMEM(attn_out.shape, BF16),
            pltpu.VMEM(d_hid.shape, BF16),
            pltpu.SemaphoreType.DMA((tiles,)),
            pltpu.SemaphoreType.DMA((2,)),
            pltpu.SemaphoreType.DMA((2,)),
            pltpu.SemaphoreType.DMA((2, 2 * tiles)),
            pltpu.SemaphoreType.DMA((2, 2 * tiles)),
            pltpu.SemaphoreType.DMA((2,)),
        ],
        compiler_params=pltpu.CompilerParams(vmem_limit_bytes=VMEM_LIMIT),
        name="weight_grads",
    )(ht, gq, gk, dwo, dwv, attn_out, d_hid, d_lnw)


def solution(mesh):
    n_dev = mesh.shape['sp']
    row_spec = P(('dp', 'sp'), None)
    full_spec = P(None, None)
    grad_spec = P('dp', None)

    def local_step(hidden, positions, d_attn, ln_weight, w_q, w_k, w_v, w_o):
        parts = run_main(n_dev, hidden, d_attn, positions, ln_weight, w_q, w_k, w_v, w_o)
        dwq, dwk, dwo, dwv, attn_out, d_hid, d_lnw = run_grads(*parts)
        return attn_out, d_hid, d_lnw, dwq, dwk, dwv, dwo

    return jax.shard_map(local_step, mesh=mesh,
                         in_specs=(row_spec, P(('dp', 'sp')), row_spec, P(None), full_spec, full_spec, full_spec, full_spec),
                         out_specs=(row_spec, row_spec, P('dp'), grad_spec, grad_spec, grad_spec, grad_spec),
                         check_vma=False)
```

```python
import functools

import jax
import jax.numpy as jnp
import numpy as np
from jax import lax
from jax.experimental import pallas as pl
from jax.experimental.pallas import tpu as pltpu
from jax.sharding import PartitionSpec as P

HEAD_DIM = 128
LN_EPS = 1e-5
ROPE_BASE = 10000.0
SCALE = HEAD_DIM ** -0.5
LOG2E = 1.4426950408889634
CORES = 2
QB = 256
MT = 512
NT = 1024
VMEM_LIMIT = 67043328
MESH = pl.DeviceIdType.MESH
F32 = jnp.float32
BF16 = jnp.bfloat16


def normalize(x):
    x = x.astype(F32)
    centered = x - jnp.mean(x, axis=-1, keepdims=True)
    rstd = lax.rsqrt(jnp.mean(centered * centered, axis=-1, keepdims=True) + LN_EPS)
    return centered * rstd, rstd


def sin_cos(a):
    n = jnp.floor(a * 0.6366197723675814 + 0.5)
    r = ((a - n * 1.5703125) - n * 4.8375129699707031e-4) - n * 7.5497899548918821e-8
    z = r * r
    s = r + r * z * (-1.6666654611e-1 + z * (8.3321608736e-3 + z * -1.9515295891e-4))
    c = 1.0 - 0.5 * z + z * z * (4.166664568298827e-2 + z * (-1.388731625493765e-3 + z * 2.443315711809948e-5))
    quad = n.astype(jnp.int32)
    odd = (quad & 1) == 1
    sin = jnp.where(odd, c, s)
    cos = jnp.where(odd, s, c)
    return jnp.where((quad & 2) == 2, -sin, sin), jnp.where(((quad + 1) & 2) == 2, -cos, cos)


def even_lanes(shape):
    return lax.broadcasted_iota(jnp.int32, shape, 1) % 2 == 0


def swap_pairs(y):
    return jnp.where(even_lanes(y.shape), pltpu.roll(y, HEAD_DIM - 1, 1), pltpu.roll(y, 1, 1))


def nt(a, b):
    return lax.dot_general(a, b, (((1,), (1,)), ((), ())), preferred_element_type=F32)


def nn(a, b):
    return jnp.dot(a, b, preferred_element_type=F32)


def main_kernel(n_dev, x_ref, g_ref, p_ref, f_ref, w_ref, wq, wk, wv, wo,
                ht_out, dwo_out, gq_out, gk_out, dwv_out, a_out, dx_out, dl_out,
                h_all, g_all, pos, cos_s, sin_s, w3, wo_s, wot_s, qkv, do_s,
                ot_s, res, m_s, li_s, kt_s, vt_s, pt_s, dst_s, a_part, a_recv, dh_part, dh_recv, cols_s, dl_buf,
                ssem, rsem, wsem, lsem, xsem, osem, psem, dsem, fsem):
    blk, model = x_ref.shape
    half = blk // 2
    rows_chip = CORES * blk
    n_chips = n_dev // CORES
    heads = qkv.shape[1]
    width = heads * HEAD_DIM
    seq = n_dev * blk
    nq = seq // QB

    me = lax.axis_index("sp")
    chip, core = me // CORES, lax.rem(me, CORES)
    other = 1 - core

    def dev(step, cr):
        return lax.rem(chip + step + n_chips, n_chips) * CORES + cr

    partner, right, left = dev(0, other), dev(1, core), dev(-1, core)
    others = [lax.rem(me + k, n_dev) for k in range(1, n_dev)]

    barrier = pltpu.get_barrier_semaphore()
    for d in others:
        pl.semaphore_signal(barrier, inc=1, device_id={"sp": d}, device_id_type=MESH)

    col0 = pl.multiple_of(core * width, width)
    wcopies = [
        pltpu.make_async_copy(w.at[:, pl.ds(col0, width)], w3.at[j], wsem.at[j])
        for j, w in enumerate((wq, wk, wv))
    ]
    wcopies.append(pltpu.make_async_copy(wo.at[pl.ds(col0, width), :], wo_s, wsem.at[3]))
    for c in wcopies:
        c.start()

    own = pl.ds(pl.multiple_of(me * blk, blk), blk)
    ln_w = w_ref[...].astype(F32).reshape(1, model)
    h_all[own, :] = (normalize(x_ref[...])[0] * ln_w).astype(BF16)
    g_all[own, :] = g_ref[...]
    pos[me] = p_ref[...].reshape(1, blk)

    arrays = (h_all, g_all)

    def region(block, piece):
        if piece is None:
            return pl.ds(pl.multiple_of(block * blk, blk), blk)
        return pl.ds(pl.multiple_of(block * blk + piece * half, half), half)

    def copy(a, kind, block, piece, to):
        r = region(block, piece)
        return pltpu.make_async_remote_copy(
            src_ref=arrays[a].at[r, :], dst_ref=arrays[a].at[r, :],
            send_sem=ssem.at[a, kind], recv_sem=rsem.at[a, kind],
            device_id={"sp": to}, device_id_type=MESH)

    far = 2
    sends = {
        0: (me, None, partner),
        1: (me, 0, right), 2: (me, 1, right),
        3: (me, 0, left), 4: (me, 1, left),
        5: (dev(-1, core), 0, right), 6: (dev(1, core), 1, left),
        7: (dev(-1, core), 0, partner), 8: (dev(-1, core), 1, partner),
        9: (dev(1, core), 0, partner), 10: (dev(1, core), 1, partner),
        11: (dev(far, core), 0, partner), 12: (dev(far, core), 1, partner),
    }
    recvs = {
        0: (partner, None),
        1: (dev(-1, core), 0), 2: (dev(-1, core), 1),
        3: (dev(1, core), 0), 4: (dev(1, core), 1),
        5: (dev(far, core), 0), 6: (dev(far, core), 1),
        7: (dev(-1, other), 0), 8: (dev(-1, other), 1),
        9: (dev(1, other), 0), 10: (dev(1, other), 1),
        11: (dev(far, other), 0), 12: (dev(far, other), 1),
    }

    def send(a, kind):
        block, piece, to = sends[kind]
        copy(a, kind, block, piece, to).start()

    def got(a, kind):
        block, piece = recvs[kind]
        copy(a, kind, block, piece, partner).wait_recv()

    def small(buf, sems, k, source, to):
        return pltpu.make_async_remote_copy(
            src_ref=buf.at[source], dst_ref=buf.at[source],
            send_sem=sems.at[0, k], recv_sem=sems.at[1, k],
            device_id={"sp": to}, device_id_type=MESH)

    def small_send(buf, sems):
        for k in range(1, n_dev):
            small(buf, sems, k, me, others[k - 1]).start()

    def small_wait(buf, sems):
        for k in range(1, n_dev):
            small(buf, sems, k, lax.rem(me - k + n_dev, n_dev), partner).wait_recv()
        for k in range(1, n_dev):
            small(buf, sems, k, me, partner).wait_send()

    pl.semaphore_wait(barrier, n_dev - 1)
    small_send(pos, psem)
    for kind in (1, 4, 2, 3, 0):
        send(0, kind)
    send(1, 0)

    def pass_first(a):
        got(a, 1)
        send(a, 5)
        send(a, 7)
        got(a, 4)
        send(a, 6)
        send(a, 10)

    def pass_second(a):
        got(a, 2)
        send(a, 8)
        got(a, 3)
        send(a, 9)

    def pass_far(a):
        got(a, 5)
        send(a, 11)
        got(a, 6)
        send(a, 12)

    def from_partner(a, which):
        for kind in which:
            got(a, kind)

    def chip_rows(i):
        step = lax.rem(i * (i + 1) // 2, n_chips)
        return pl.ds(pl.multiple_of(lax.rem(chip + step, n_chips) * rows_chip, rows_chip), rows_chip)

    def fill_tables():
        small_wait(pos, psem)
        diag = (lax.broadcasted_iota(jnp.int32, (blk, blk), 0)
                == lax.broadcasted_iota(jnp.int32, (blk, blk), 1))
        even = even_lanes((blk, HEAD_DIM))

        @pl.loop(0, n_dev)
        def _(b):
            r = pl.ds(pl.multiple_of(b * blk, blk), blk)
            p = jnp.broadcast_to(pos[b].astype(F32), (blk, blk))
            col = jnp.sum(jnp.where(diag, p, 0.0), axis=1, keepdims=True)
            sin, cos = sin_cos(col * f_ref[...])
            cos_s[r, :] = cos
            sin_s[r, :] = jnp.where(even, -sin, sin)

    def project_do(r):
        for part in range(0, heads, 4):
            y = nn(g_all[r, :], wot_s[:, part * HEAD_DIM:(part + 4) * HEAD_DIM])
            for n in range(4):
                do_s[part + n, r, :] = y[:, n * HEAD_DIM:(n + 1) * HEAD_DIM].astype(BF16)

    def job_rows(i):
        mid, late = (lax.rem(i, 3) + 1) // 2, i // 2
        runs = []
        for k in range(4):
            beside = (n_chips - 1, half * late + blk * k) if k < 2 else (1, half * (1 - late) + blk * (k - 2))
            step = (1 - mid) * (i // 3) * far + mid * beside[0]
            row = lax.rem(chip + step, n_chips) * rows_chip + (1 - mid) * half * k + mid * beside[1]
            runs.append(pl.ds(pl.multiple_of(row, half), half))
        return runs

    @pl.loop(0, n_chips)
    def _(i):
        @pl.when(i == 0)
        def _():
            fill_tables()
            got(0, 0)
            for c in wcopies:
                c.wait()

        @pl.when(i == 1)
        def _():
            for e in range(width // QB):
                wot_s[:, e * QB:(e + 1) * QB] = wo_s[e * QB:(e + 1) * QB, :].T
            got(1, 0)
            project_do(chip_rows(0))
            pass_first(0)
            for kind in (1, 4, 2, 3):
                send(1, kind)
            from_partner(0, (7, 10))

        @pl.when(i == 2)
        def _():
            pass_second(0)
            from_partner(0, (8, 9))

        @pl.when(i == 3)
        def _():
            pass_far(0)
            from_partner(0, (11, 12))

        runs = job_rows(i)

        def rows_of(ref):
            return jnp.concatenate([ref[r, :] for r in runs], axis=0)

        x = rows_of(h_all)
        c, s = rows_of(cos_s), rows_of(sin_s)
        for j in range(3):
            for part in range(0, heads, 4):
                y = nn(x, w3[j, :, part * HEAD_DIM:(part + 4) * HEAD_DIM])
                for n in range(4):
                    yn = y[:, n * HEAD_DIM:(n + 1) * HEAD_DIM]
                    yn = (yn if j == 2 else yn * c + swap_pairs(yn) * s).astype(BF16)
                    for k, r in enumerate(runs):
                        qkv[j, part + n, r, :] = yn[k * half:(k + 1) * half]


    outs = (dwo_out, gq_out, gk_out, dwv_out)
    my_col = core * width

    def give(a, src, dst):
        pltpu.make_async_copy(src, dst, osem.at[a]).start()
        pltpu.make_async_remote_copy(
            src_ref=src, dst_ref=dst, send_sem=xsem.at[0, a], recv_sem=xsem.at[1, a],
            device_id={"sp": partner}, device_id_type=MESH).start()

    def head_cols(n):
        return pl.ds(pl.multiple_of(my_col + n * HEAD_DIM, HEAD_DIM), HEAD_DIM)

    def rows_tile(m, size=QB):
        return pl.ds(pl.multiple_of(m * size, size), size)

    def in_turn(streams):
        while streams:
            for g in list(streams):
                if next(g, None) is None:
                    streams.remove(g)

    c2 = SCALE * LOG2E
    causal = (lax.broadcasted_iota(jnp.int32, (QB, QB), 0)
              <= lax.broadcasted_iota(jnp.int32, (QB, QB), 1))

    def tile(i):
        return slice(i * QB, (i + 1) * QB)

    def scores(n, i, j):
        s = nt(qkv[1, n, tile(j), :], qkv[0, n, tile(i), :])
        return jnp.where(causal, s, -jnp.inf) if i == j else s

    def forward(n, slot):
        vt = vt_s.at[slot]
        vt[...] = qkv[2, n].T
        for i in range(nq):
            ss = [scores(n, i, j) for j in range(i + 1)]
            yield True
            m = functools.reduce(jnp.maximum, [jnp.max(s, axis=0, keepdims=True) for s in ss])
            es = [jnp.exp2((s - m) * c2) for s in ss]
            li = 1.0 / sum(jnp.sum(e, axis=0, keepdims=True) for e in es)
            m_s[n, :, tile(i)] = m
            li_s[n, :, tile(i)] = li
            ps = [(e * li).astype(BF16) for e in es]
            yield True
            ot_s[n, :, tile(i)] = sum(nn(vt[:, tile(j)], p) for j, p in enumerate(ps)).astype(BF16)
            yield True

    @pl.loop(0, heads // 2)
    def _(t):
        @pl.when(t == 1)
        def _():
            pass_first(1)

        in_turn([forward(2 * t, 0), forward(2 * t + 1, 1)])

    here = pl.ds(pl.multiple_of(chip * rows_chip, rows_chip), rows_chip)
    mine = pl.ds(pl.multiple_of(core * blk, blk), blk)
    theirs = pl.ds(pl.multiple_of(other * blk, blk), blk)

    def swap_part(src, recv, k):
        return pltpu.make_async_remote_copy(
            src_ref=src, dst_ref=recv, send_sem=fsem.at[0, k], recv_sem=fsem.at[1, k],
            device_id={"sp": partner}, device_id_type=MESH)

    a_swap = swap_part(a_part.at[theirs, :], a_recv, 0)

    @pl.loop(1, n_chips)
    def _(i):
        @pl.when(i == 1)
        def _():
            pass_second(1)
            from_partner(1, (7, 8, 9, 10))

        @pl.when(i == 3)
        def _():
            o_here = jnp.concatenate([ot_s[n, :, here] for n in range(heads)], axis=0).T
            for n in range(0, model, NT):
                a_part[:, n:n + NT] = nn(o_here, wo_s[:, n:n + NT])
            a_swap.start()
            pass_far(1)
            from_partner(1, (11, 12))

        project_do(chip_rows(i))

    for kind, (block, piece, to) in sends.items():
        copy(0, kind, block, piece, to).wait_send()
    for e in range(0, model, QB):
        wot_s[e:e + QB, :] = h_all[:, e:e + QB].T
    ht_copy = pltpu.make_async_copy(wot_s, ht_out, lsem.at[0])
    ht_copy.start()

    def at(j, i):
        return i * (i + 1) // 2 + j

    def backward(n, slot):
        kt, pt, dst = kt_s.at[slot], pt_s.at[slot], dst_s.at[slot]
        kt[...] = qkv[1, n].T
        for i in reversed(range(nq)):
            q_i, do_i = qkv[0, n, tile(i), :], do_s[n, tile(i), :]
            ss = [scores(n, i, j) for j in range(i + 1)]
            dps = [nt(qkv[2, n, tile(j), :], do_i) for j in range(i + 1)]
            yield True
            m, li = m_s[n, :, tile(i)], li_s[n, :, tile(i)]
            ps = [jnp.exp2((s - m) * c2) * li for s in ss]
            ts = [p * dp for p, dp in zip(ps, dps)]
            rdot = sum(jnp.sum(t, axis=0, keepdims=True) for t in ts)
            for j in range(i + 1):
                pt[at(j, i)] = ps[j].astype(BF16)
                dst[at(j, i)] = ((ts[j] - ps[j] * rdot) * SCALE).astype(BF16)
            yield True
            dq = sum(nn(kt[:, tile(j)], dst[at(j, i)]) for j in range(i + 1)).T.astype(BF16).astype(F32)
            c, s = cos_s[tile(i), :], sin_s[tile(i), :]
            res[0, n, tile(i), :] = (dq * c - swap_pairs(dq) * s).astype(BF16)
            dk = sum(nn(dst[at(i, k)], qkv[0, n, tile(k), :]) for k in range(i, nq)).astype(BF16).astype(F32)
            res[1, n, tile(i), :] = (dk * c - swap_pairs(dk) * s).astype(BF16)
            res[2, n, tile(i), :] = sum(nn(pt[at(i, k)], do_s[n, tile(k), :]) for k in range(i, nq)).astype(BF16)
            yield True

    def out_grad(t):
        o_t = jnp.concatenate([ot_s[2 * t], ot_s[2 * t + 1]], axis=0)
        for n in range(0, model, QB):
            h_all[rows_tile(t), n:n + QB] = nn(o_t, g_all[:, n:n + QB]).astype(BF16)
            yield True

    @pl.loop(0, heads // 2)
    def _(t):
        in_turn([backward(2 * t, 0), backward(2 * t + 1, 1), out_grad(t)])
        give(0, h_all.at[rows_tile(t), :], dwo_out.at[pl.ds(pl.multiple_of(my_col + t * QB, QB), QB), :])
        for a in (1, 2):
            for n in (2 * t, 2 * t + 1):
                give(a, res.at[a - 1, n], outs[a].at[:, head_cols(n)])

    def cols_of(j):
        return jnp.concatenate([res[j, n, here, :] for n in range(heads)], axis=1).T

    for j in range(3):
        cols_s[j] = cols_of(j)

    @pl.loop(0, model // MT)
    def _(d):
        r = pl.ds(pl.multiple_of(d * MT, MT), MT)
        dh_t = sum(nn(w3[j, r, :], cols_s[j]) for j in range(3))
        for k in range(CORES):
            dh_part[k, r, :] = dh_t[:, k * blk:(k + 1) * blk]

    dh_swap = swap_part(dh_part.at[other], dh_recv, 1)
    dh_swap.start()

    def finish_rows():
        a_swap.wait()
        a_out[...] = (a_part[mine, :] + a_recv[...]).astype(BF16)
        xhat, rstd = normalize(x_ref[...])
        dh_swap.wait()
        dh = (dh_part[core] + dh_recv[...]).T
        dl_buf[me] = jnp.sum(dh * xhat, axis=0, keepdims=True)
        small_send(dl_buf, dsem)
        dy = dh * ln_w
        dx = dy - jnp.mean(dy, axis=-1, keepdims=True) - xhat * jnp.mean(dy * xhat, axis=-1, keepdims=True)
        dx_out[...] = (dx * rstd).astype(BF16)

    @pl.loop(0, model // MT)
    def _(m):
        @pl.when(m == 2)
        def _():
            finish_rows()

        per = seq // MT
        place = pl.ds(pl.multiple_of(lax.rem(m, per) * MT, MT), MT)
        for part in range(0, heads, 4):
            gv = jnp.concatenate([res[2, part + n] for n in range(4)], axis=1)
            y = nn(wot_s[rows_tile(m, MT), :], gv).astype(BF16)
            for n in range(4):
                qkv[m // per, part + n, place, :] = y[:, n * HEAD_DIM:(n + 1) * HEAD_DIM]
        for n in range(heads):
            give(3, qkv.at[m // per, n, place, :], dwv_out.at[rows_tile(m, MT), head_cols(n)])

    ht_copy.wait()
    for kind, (block, piece, to) in sends.items():
        copy(1, kind, block, piece, to).wait_send()
    my_span = pl.ds(pl.multiple_of(core * width, width), width)
    their_span = pl.ds(pl.multiple_of(other * width, width), width)
    for a in range(4):
        sent = outs[a].at[my_span, :] if a == 0 else outs[a].at[:, my_span]
        came = outs[a].at[their_span, :] if a == 0 else outs[a].at[:, their_span]
        pltpu.make_async_copy(sent, sent, osem.at[a]).wait()
        done = pltpu.make_async_remote_copy(
            src_ref=sent, dst_ref=came, send_sem=xsem.at[0, a], recv_sem=xsem.at[1, a],
            device_id={"sp": partner}, device_id_type=MESH)
        done.wait_send()
        done.wait_recv()
    small_wait(dl_buf, dsem)
    total = dl_buf[0]
    for k in range(1, n_dev):
        total = total + dl_buf[k]
    dl_out[...] = total.astype(BF16).reshape(model)


def run_main(n_dev, hidden, d_attn, positions, ln_weight, w_q, w_k, w_v, w_o):
    blk, model = hidden.shape
    seq = n_dev * blk
    width = w_q.shape[1] // CORES
    heads = width // HEAD_DIM
    pairs = (seq // QB) * (seq // QB + 1) // 2
    vm = pl.BlockSpec(memory_space=pltpu.VMEM)
    hbm = pl.BlockSpec(memory_space=pl.ANY)
    full = w_q.shape[1]
    wide = jax.ShapeDtypeStruct((seq, full), BF16)
    rows = jax.ShapeDtypeStruct((blk, model), BF16)
    freq = np.repeat(ROPE_BASE ** (-np.arange(0, HEAD_DIM, 2) / HEAD_DIM), 2)[None, :].astype(np.float32)
    return pl.pallas_call(
        functools.partial(main_kernel, n_dev),
        out_shape=(jax.ShapeDtypeStruct((model, seq), BF16), jax.ShapeDtypeStruct((full, model), BF16),
                   wide, wide, jax.ShapeDtypeStruct((model, full), BF16), rows, rows, jax.ShapeDtypeStruct((model,), BF16)),
        in_specs=[vm] * 5 + [hbm] * 4,
        out_specs=[hbm] * 5 + [vm] * 3,
        scratch_shapes=[
            pltpu.VMEM((seq, model), BF16),
            pltpu.VMEM((seq, model), BF16),
            pltpu.VMEM((n_dev, 1, blk), jnp.int32),
            pltpu.VMEM((seq, HEAD_DIM), F32),
            pltpu.VMEM((seq, HEAD_DIM), F32),
            pltpu.VMEM((3, model, width), BF16),
            pltpu.VMEM((width, model), BF16),
            pltpu.VMEM((model, width), BF16),
            pltpu.VMEM((3, heads, seq, HEAD_DIM), BF16),
            pltpu.VMEM((heads, seq, HEAD_DIM), BF16),
            pltpu.VMEM((heads, HEAD_DIM, seq), BF16),
            pltpu.VMEM((3, heads, seq, HEAD_DIM), BF16),
            pltpu.VMEM((heads, 1, seq), F32),
            pltpu.VMEM((heads, 1, seq), F32),
            pltpu.VMEM((2, HEAD_DIM, seq), BF16),
            pltpu.VMEM((2, HEAD_DIM, seq), BF16),
            pltpu.VMEM((2, pairs, QB, QB), BF16),
            pltpu.VMEM((2, pairs, QB, QB), BF16),
            pltpu.VMEM((CORES * blk, model), F32),
            pltpu.VMEM((blk, model), F32),
            pltpu.VMEM((CORES, model, blk), F32),
            pltpu.VMEM((model, blk), F32),
            pltpu.VMEM((3, width, CORES * blk), BF16),
            pltpu.VMEM((n_dev, 1, model), F32),
            pltpu.SemaphoreType.DMA((2, 13)),
            pltpu.SemaphoreType.DMA((2, 13)),
            pltpu.SemaphoreType.DMA((4,)),
            pltpu.SemaphoreType.DMA((1,)),
            pltpu.SemaphoreType.DMA((2, 4)),
            pltpu.SemaphoreType.DMA((4,)),
            pltpu.SemaphoreType.DMA((2, n_dev)),
            pltpu.SemaphoreType.DMA((2, n_dev)),
            pltpu.SemaphoreType.DMA((2, 2)),
        ],
        compiler_params=pltpu.CompilerParams(
            collective_id=0, has_side_effects=True, vmem_limit_bytes=VMEM_LIMIT),
        name="gather_attention",
    )(hidden, d_attn, positions, freq, ln_weight, w_q, w_k, w_v, w_o)


def grad_kernel(ht, gq, gk, dwo_in, dwv_in, a_in, dx_in, dl_in,
                dq_out, dk_out, dwo_out, dwv_out, a_out, dx_out, dl_out,
                ht_v, g2, out_v, dwo_v, dwv_v, a_v, dx_v, hsem, gsem, usem, isem, osem, rsem):
    tiles = ht.shape[0] // MT
    steps = 2 * tiles
    wide = gq.shape[1]
    part = dwo_in.shape[0] // steps
    outs = (dq_out, dk_out)

    def rows(m, size=MT):
        return pl.ds(pl.multiple_of(m * size, size), size)

    ht_loads = [pltpu.make_async_copy(ht.at[rows(m), :], ht_v.at[rows(m), :], hsem.at[m]) for m in range(tiles)]
    g_loads = [pltpu.make_async_copy(x, g2.at[k], gsem.at[k]) for k, x in enumerate((gq, gk))]
    row_in = [pltpu.make_async_copy(a_in, a_v, rsem.at[0]), pltpu.make_async_copy(dx_in, dx_v, rsem.at[1])]
    row_out = [pltpu.make_async_copy(a_v, a_out, rsem.at[0]), pltpu.make_async_copy(dx_v, dx_out, rsem.at[1])]

    def bring(k, it):
        src, buf = ((dwo_in, dwo_v), (dwv_in, dwv_v))[k]
        return pltpu.make_async_copy(src.at[rows(it, part), :], buf.at[rows(it, part), :], isem.at[k, it])

    def put(k, it):
        buf, dst = ((dwo_v, dwo_out), (dwv_v, dwv_out))[k]
        return pltpu.make_async_copy(buf.at[rows(it, part), :], dst.at[rows(it, part), :], osem.at[k, it])

    def store(slot, out, m):
        return pltpu.make_async_copy(out_v.at[slot], out.at[rows(m), :], usem.at[slot])

    ht_loads[0].start()
    g_loads[0].start()
    for c in ht_loads[1:] + g_loads[1:] + row_in:
        c.start()
    for k in range(2):
        bring(k, 0).start()
    dl_out[...] = dl_in[...]

    @pl.loop(0, steps)
    def _(it):
        k, m, slot = it // tiles, lax.rem(it, tiles), lax.rem(it, 2)
        for j in range(tiles):
            @pl.when(it == j)
            def _():
                ht_loads[j].wait()
        for j in range(2):
            @pl.when(it == j * tiles)
            def _():
                g_loads[j].wait()

        @pl.when(it == 1)
        def _():
            for c, d in zip(row_in, row_out):
                c.wait()
                d.start()

        @pl.when(it >= 2)
        def _():
            store(slot, dq_out, 0).wait()

        for n in range(0, wide, NT):
            out_v[slot, :, n:n + NT] = nn(ht_v[rows(m), :], g2[k, :, n:n + NT]).astype(BF16)
        for j in range(2):
            @pl.when(k == j)
            def _():
                store(slot, outs[j], m).start()
            bring(j, it).wait()
            put(j, it).start()

            @pl.when(it < steps - 1)
            def _():
                bring(j, it + 1).start()

    for slot in range(2):
        store(slot, dq_out, 0).wait()
    for it in range(steps):
        for k in range(2):
            put(k, it).wait()
    for d in row_out:
        d.wait()


def run_grads(ht, dwo, gq, gk, dwv, attn_out, d_hid, d_lnw):
    model, seq = ht.shape
    wide = gq.shape[1]
    tiles = model // MT
    hbm = pl.BlockSpec(memory_space=pl.ANY)
    vm = pl.BlockSpec(memory_space=pltpu.VMEM)

    def like(a):
        return jax.ShapeDtypeStruct(a.shape, a.dtype)

    grad = jax.ShapeDtypeStruct((model, wide), BF16)
    return pl.pallas_call(
        grad_kernel,
        out_shape=[grad, grad, like(dwo), like(dwv), like(attn_out), like(d_hid), like(d_lnw)],
        in_specs=[hbm] * 7 + [vm],
        out_specs=[hbm] * 6 + [vm],
        scratch_shapes=[
            pltpu.VMEM((model, seq), BF16),
            pltpu.VMEM((2, seq, wide), BF16),
            pltpu.VMEM((2, MT, wide), BF16),
            pltpu.VMEM(dwo.shape, BF16),
            pltpu.VMEM(dwv.shape, BF16),
            pltpu.VMEM(attn_out.shape, BF16),
            pltpu.VMEM(d_hid.shape, BF16),
            pltpu.SemaphoreType.DMA((tiles,)),
            pltpu.SemaphoreType.DMA((2,)),
            pltpu.SemaphoreType.DMA((2,)),
            pltpu.SemaphoreType.DMA((2, 2 * tiles)),
            pltpu.SemaphoreType.DMA((2, 2 * tiles)),
            pltpu.SemaphoreType.DMA((2,)),
        ],
        compiler_params=pltpu.CompilerParams(vmem_limit_bytes=VMEM_LIMIT),
        name="weight_grads",
    )(ht, gq, gk, dwo, dwv, attn_out, d_hid, d_lnw)


def solution(mesh):
    n_dev = mesh.shape['sp']
    row_spec = P(('dp', 'sp'), None)
    full_spec = P(None, None)
    grad_spec = P('dp', None)

    def local_step(hidden, positions, d_attn, ln_weight, w_q, w_k, w_v, w_o):
        parts = run_main(n_dev, hidden, d_attn, positions, ln_weight, w_q, w_k, w_v, w_o)
        dwq, dwk, dwo, dwv, attn_out, d_hid, d_lnw = run_grads(*parts)
        return attn_out, d_hid, d_lnw, dwq, dwk, dwv, dwo

    return jax.shard_map(local_step, mesh=mesh,
                         in_specs=(row_spec, P(('dp', 'sp')), row_spec, P(None), full_spec, full_spec, full_spec, full_spec),
                         out_specs=(row_spec, row_spec, P('dp'), grad_spec, grad_spec, grad_spec, grad_spec),
                         check_vma=False)
```

```python
import functools

import jax
import jax.numpy as jnp
import numpy as np
from jax import lax
from jax.experimental import pallas as pl
from jax.experimental.pallas import tpu as pltpu
from jax.sharding import PartitionSpec as P

HEAD_DIM = 128
LN_EPS = 1e-5
ROPE_BASE = 10000.0
SCALE = HEAD_DIM ** -0.5
LOG2E = 1.4426950408889634
CORES = 2
QB = 256
MT = 512
NT = 1024
VMEM_LIMIT = 67043328
MESH = pl.DeviceIdType.MESH
F32 = jnp.float32
BF16 = jnp.bfloat16


def normalize(x):
    x = x.astype(F32)
    centered = x - jnp.mean(x, axis=-1, keepdims=True)
    rstd = lax.rsqrt(jnp.mean(centered * centered, axis=-1, keepdims=True) + LN_EPS)
    return centered * rstd, rstd


def sin_cos(a):
    n = jnp.floor(a * 0.6366197723675814 + 0.5)
    r = ((a - n * 1.5703125) - n * 4.8375129699707031e-4) - n * 7.5497899548918821e-8
    z = r * r
    s = r + r * z * (-1.6666654611e-1 + z * (8.3321608736e-3 + z * -1.9515295891e-4))
    c = 1.0 - 0.5 * z + z * z * (4.166664568298827e-2 + z * (-1.388731625493765e-3 + z * 2.443315711809948e-5))
    quad = n.astype(jnp.int32)
    odd = (quad & 1) == 1
    sin = jnp.where(odd, c, s)
    cos = jnp.where(odd, s, c)
    return jnp.where((quad & 2) == 2, -sin, sin), jnp.where(((quad + 1) & 2) == 2, -cos, cos)


def even_lanes(shape):
    return lax.broadcasted_iota(jnp.int32, shape, 1) % 2 == 0


def swap_pairs(y):
    return jnp.where(even_lanes(y.shape), pltpu.roll(y, HEAD_DIM - 1, 1), pltpu.roll(y, 1, 1))


def nt(a, b):
    return lax.dot_general(a, b, (((1,), (1,)), ((), ())), preferred_element_type=F32)


def nn(a, b):
    return jnp.dot(a, b, preferred_element_type=F32)


def main_kernel(n_dev, x_ref, g_ref, p_ref, f_ref, w_ref, wq, wk, wv, wo,
                ht_out, dwo_out, gq_out, gk_out, dwv_out, a_out, dx_out, dl_out,
                h_all, g_all, pos, cos_s, sin_s, w3, wo_s, wot_s, qkv, do_s,
                ot_s, res, m_s, li_s, kt_s, vt_s, pt_s, dst_s, a_part, a_recv, dh_part, dh_recv, cols_s, dl_buf,
                ssem, rsem, wsem, lsem, xsem, osem, psem, dsem, fsem):
    blk, model = x_ref.shape
    half = blk // 2
    rows_chip = CORES * blk
    n_chips = n_dev // CORES
    heads = qkv.shape[1]
    width = heads * HEAD_DIM
    seq = n_dev * blk
    nq = seq // QB

    me = lax.axis_index("sp")
    chip, core = me // CORES, lax.rem(me, CORES)
    other = 1 - core

    def dev(step, cr):
        return lax.rem(chip + step + n_chips, n_chips) * CORES + cr

    partner, right, left = dev(0, other), dev(1, core), dev(-1, core)
    others = [lax.rem(me + k, n_dev) for k in range(1, n_dev)]

    barrier = pltpu.get_barrier_semaphore()
    for d in others:
        pl.semaphore_signal(barrier, inc=1, device_id={"sp": d}, device_id_type=MESH)

    col0 = pl.multiple_of(core * width, width)
    wcopies = [
        pltpu.make_async_copy(w.at[:, pl.ds(col0, width)], w3.at[j], wsem.at[j])
        for j, w in enumerate((wq, wk, wv))
    ]
    wcopies.append(pltpu.make_async_copy(wo.at[pl.ds(col0, width), :], wo_s, wsem.at[3]))
    for c in wcopies:
        c.start()

    own = pl.ds(pl.multiple_of(me * blk, blk), blk)
    ln_w = w_ref[...].astype(F32).reshape(1, model)
    h_all[own, :] = (normalize(x_ref[...])[0] * ln_w).astype(BF16)
    g_all[own, :] = g_ref[...]
    pos[me] = p_ref[...].reshape(1, blk)

    arrays = (h_all, g_all)

    def region(block, piece):
        if piece is None:
            return pl.ds(pl.multiple_of(block * blk, blk), blk)
        return pl.ds(pl.multiple_of(block * blk + piece * half, half), half)

    def copy(a, kind, block, piece, to):
        r = region(block, piece)
        return pltpu.make_async_remote_copy(
            src_ref=arrays[a].at[r, :], dst_ref=arrays[a].at[r, :],
            send_sem=ssem.at[a, kind], recv_sem=rsem.at[a, kind],
            device_id={"sp": to}, device_id_type=MESH)

    far = 2
    sends = {
        0: (me, None, partner),
        1: (me, 0, right), 2: (me, 1, right),
        3: (me, 0, left), 4: (me, 1, left),
        5: (dev(-1, core), 0, right), 6: (dev(1, core), 1, left),
        7: (dev(-1, core), 0, partner), 8: (dev(-1, core), 1, partner),
        9: (dev(1, core), 0, partner), 10: (dev(1, core), 1, partner),
        11: (dev(far, core), 0, partner), 12: (dev(far, core), 1, partner),
    }
    recvs = {
        0: (partner, None),
        1: (dev(-1, core), 0), 2: (dev(-1, core), 1),
        3: (dev(1, core), 0), 4: (dev(1, core), 1),
        5: (dev(far, core), 0), 6: (dev(far, core), 1),
        7: (dev(-1, other), 0), 8: (dev(-1, other), 1),
        9: (dev(1, other), 0), 10: (dev(1, other), 1),
        11: (dev(far, other), 0), 12: (dev(far, other), 1),
    }

    def send(a, kind):
        block, piece, to = sends[kind]
        copy(a, kind, block, piece, to).start()

    def got(a, kind):
        block, piece = recvs[kind]
        copy(a, kind, block, piece, partner).wait_recv()

    def small(buf, sems, k, source, to):
        return pltpu.make_async_remote_copy(
            src_ref=buf.at[source], dst_ref=buf.at[source],
            send_sem=sems.at[0, k], recv_sem=sems.at[1, k],
            device_id={"sp": to}, device_id_type=MESH)

    def small_send(buf, sems):
        for k in range(1, n_dev):
            small(buf, sems, k, me, others[k - 1]).start()

    def small_wait(buf, sems):
        for k in range(1, n_dev):
            small(buf, sems, k, lax.rem(me - k + n_dev, n_dev), partner).wait_recv()
        for k in range(1, n_dev):
            small(buf, sems, k, me, partner).wait_send()

    pl.semaphore_wait(barrier, n_dev - 1)
    small_send(pos, psem)
    for kind in (1, 4, 2, 3, 0):
        send(0, kind)
    send(1, 0)

    def pass_first(a):
        got(a, 1)
        send(a, 5)
        send(a, 7)
        got(a, 4)
        send(a, 6)
        send(a, 10)

    def pass_second(a):
        got(a, 2)
        send(a, 8)
        got(a, 3)
        send(a, 9)

    def pass_far(a):
        got(a, 5)
        send(a, 11)
        got(a, 6)
        send(a, 12)

    def from_partner(a, which):
        for kind in which:
            got(a, kind)

    def chip_rows(i):
        step = lax.rem(i * (i + 1) // 2, n_chips)
        return pl.ds(pl.multiple_of(lax.rem(chip + step, n_chips) * rows_chip, rows_chip), rows_chip)

    def fill_tables():
        small_wait(pos, psem)
        diag = (lax.broadcasted_iota(jnp.int32, (blk, blk), 0)
                == lax.broadcasted_iota(jnp.int32, (blk, blk), 1))
        even = even_lanes((blk, HEAD_DIM))

        @pl.loop(0, n_dev)
        def _(b):
            r = pl.ds(pl.multiple_of(b * blk, blk), blk)
            p = jnp.broadcast_to(pos[b].astype(F32), (blk, blk))
            col = jnp.sum(jnp.where(diag, p, 0.0), axis=1, keepdims=True)
            sin, cos = sin_cos(col * f_ref[...])
            cos_s[r, :] = cos
            sin_s[r, :] = jnp.where(even, -sin, sin)

    def project_do(r):
        for part in range(0, heads, 4):
            y = nn(g_all[r, :], wot_s[:, part * HEAD_DIM:(part + 4) * HEAD_DIM])
            for n in range(4):
                do_s[part + n, r, :] = y[:, n * HEAD_DIM:(n + 1) * HEAD_DIM].astype(BF16)

    def job_rows(i):
        mid, late = (lax.rem(i, 3) + 1) // 2, i // 2
        runs = []
        for k in range(4):
            beside = (n_chips - 1, half * late + blk * k) if k < 2 else (1, half * (1 - late) + blk * (k - 2))
            step = (1 - mid) * (i // 3) * far + mid * beside[0]
            row = lax.rem(chip + step, n_chips) * rows_chip + (1 - mid) * half * k + mid * beside[1]
            runs.append(pl.ds(pl.multiple_of(row, half), half))
        return runs

    @pl.loop(0, n_chips)
    def _(i):
        @pl.when(i == 0)
        def _():
            fill_tables()
            got(0, 0)
            for c in wcopies:
                c.wait()

        @pl.when(i == 1)
        def _():
            for e in range(width // QB):
                wot_s[:, e * QB:(e + 1) * QB] = wo_s[e * QB:(e + 1) * QB, :].T
            got(1, 0)
            project_do(chip_rows(0))
            pass_first(0)
            for kind in (1, 4, 2, 3):
                send(1, kind)
            from_partner(0, (7, 10))

        @pl.when(i == 2)
        def _():
            pass_second(0)
            from_partner(0, (8, 9))

        @pl.when(i == 3)
        def _():
            pass_far(0)
            from_partner(0, (11, 12))

        runs = job_rows(i)

        def rows_of(ref):
            return jnp.concatenate([ref[r, :] for r in runs], axis=0)

        x = rows_of(h_all)
        c, s = rows_of(cos_s), rows_of(sin_s)
        for j in range(3):
            for part in range(0, heads, 4):
                y = nn(x, w3[j, :, part * HEAD_DIM:(part + 4) * HEAD_DIM])
                for n in range(4):
                    yn = y[:, n * HEAD_DIM:(n + 1) * HEAD_DIM]
                    yn = (yn if j == 2 else yn * c + swap_pairs(yn) * s).astype(BF16)
                    for k, r in enumerate(runs):
                        qkv[j, part + n, r, :] = yn[k * half:(k + 1) * half]


    outs = (dwo_out, gq_out, gk_out, dwv_out)
    my_col = core * width

    def give(a, src, dst):
        pltpu.make_async_copy(src, dst, osem.at[a]).start()
        pltpu.make_async_remote_copy(
            src_ref=src, dst_ref=dst, send_sem=xsem.at[0, a], recv_sem=xsem.at[1, a],
            device_id={"sp": partner}, device_id_type=MESH).start()

    def head_cols(n):
        return pl.ds(pl.multiple_of(my_col + n * HEAD_DIM, HEAD_DIM), HEAD_DIM)

    def rows_tile(m, size=QB):
        return pl.ds(pl.multiple_of(m * size, size), size)

    def in_turn(streams):
        while streams:
            for g in list(streams):
                if next(g, None) is None:
                    streams.remove(g)

    c2 = SCALE * LOG2E
    causal = (lax.broadcasted_iota(jnp.int32, (QB, QB), 0)
              <= lax.broadcasted_iota(jnp.int32, (QB, QB), 1))

    def tile(i):
        return slice(i * QB, (i + 1) * QB)

    def scores(n, i, j):
        s = nt(qkv[1, n, tile(j), :], qkv[0, n, tile(i), :])
        return jnp.where(causal, s, -jnp.inf) if i == j else s

    def forward(n, slot):
        vt = vt_s.at[slot]
        vt[...] = qkv[2, n].T
        ss = [scores(n, 0, 0)]
        yield True
        for i in range(nq):
            now = ss
            if i + 1 < nq:
                ss = [scores(n, i + 1, j) for j in range(i + 2)]
            yield True
            m = jnp.max(functools.reduce(jnp.maximum, now), axis=0, keepdims=True)
            es = [jnp.exp2((s - m) * c2) for s in now]
            li = 1.0 / jnp.sum(sum(es), axis=0, keepdims=True)
            m_s[n, :, tile(i)] = m
            li_s[n, :, tile(i)] = li
            ps = [(e * li).astype(BF16) for e in es]
            ot_s[n, :, tile(i)] = sum(nn(vt[:, tile(j)], p) for j, p in enumerate(ps)).astype(BF16)
            yield True

    @pl.loop(0, heads // 2)
    def _(t):
        @pl.when(t == 1)
        def _():
            pass_first(1)

        first = forward(2 * t, 0)
        next(first)
        in_turn([first, forward(2 * t + 1, 1)])

    here = pl.ds(pl.multiple_of(chip * rows_chip, rows_chip), rows_chip)
    mine = pl.ds(pl.multiple_of(core * blk, blk), blk)
    theirs = pl.ds(pl.multiple_of(other * blk, blk), blk)

    def swap_part(src, recv, k):
        return pltpu.make_async_remote_copy(
            src_ref=src, dst_ref=recv, send_sem=fsem.at[0, k], recv_sem=fsem.at[1, k],
            device_id={"sp": partner}, device_id_type=MESH)

    a_swap = swap_part(a_part.at[theirs, :], a_recv, 0)

    @pl.loop(1, n_chips)
    def _(i):
        @pl.when(i == 1)
        def _():
            pass_second(1)
            from_partner(1, (7, 8, 9, 10))

        @pl.when(i == 3)
        def _():
            o_here = jnp.concatenate([ot_s[n, :, here] for n in range(heads)], axis=0).T
            for n in range(0, model, NT):
                a_part[:, n:n + NT] = nn(o_here, wo_s[:, n:n + NT])
            a_swap.start()
            pass_far(1)
            from_partner(1, (11, 12))

        project_do(chip_rows(i))

    for kind, (block, piece, to) in sends.items():
        copy(0, kind, block, piece, to).wait_send()
    for e in range(0, model, QB):
        wot_s[e:e + QB, :] = h_all[:, e:e + QB].T
    ht_copy = pltpu.make_async_copy(wot_s, ht_out, lsem.at[0])
    ht_copy.start()

    def at(j, i):
        return i * (i + 1) // 2 + j

    def backward(n, slot):
        kt, pt, dst = kt_s.at[slot], pt_s.at[slot], dst_s.at[slot]
        kt[...] = qkv[1, n].T
        def products(i):
            q_i, do_i = qkv[0, n, tile(i), :], do_s[n, tile(i), :]
            return ([scores(n, i, j) for j in range(i + 1)],
                    [nt(qkv[2, n, tile(j), :], do_i) for j in range(i + 1)])

        ahead = products(nq - 1)
        yield True
        for i in reversed(range(nq)):
            ss, dps = ahead
            m, li = m_s[n, :, tile(i)], li_s[n, :, tile(i)]
            ps = [jnp.exp2((s - m) * c2) * li for s in ss]
            ts = [p * dp for p, dp in zip(ps, dps)]
            rdot = jnp.sum(sum(ts), axis=0, keepdims=True)
            for j in range(i + 1):
                pt[at(j, i)] = ps[j].astype(BF16)
                dst[at(j, i)] = ((ts[j] - ps[j] * rdot) * SCALE).astype(BF16)
            yield True
            if i:
                ahead = products(i - 1)
            yield True
            dq = sum(nn(kt[:, tile(j)], dst[at(j, i)]) for j in range(i + 1)).T.astype(BF16).astype(F32)
            c, s = cos_s[tile(i), :], sin_s[tile(i), :]
            res[0, n, tile(i), :] = (dq * c - swap_pairs(dq) * s).astype(BF16)
            dk = sum(nn(dst[at(i, k)], qkv[0, n, tile(k), :]) for k in range(i, nq)).astype(BF16).astype(F32)
            res[1, n, tile(i), :] = (dk * c - swap_pairs(dk) * s).astype(BF16)
            res[2, n, tile(i), :] = sum(nn(pt[at(i, k)], do_s[n, tile(k), :]) for k in range(i, nq)).astype(BF16)
            yield True

    def out_grad(t):
        o_t = jnp.concatenate([ot_s[2 * t], ot_s[2 * t + 1]], axis=0)
        for n in range(0, model, QB):
            h_all[rows_tile(t), n:n + QB] = nn(o_t, g_all[:, n:n + QB]).astype(BF16)
            yield True

    @pl.loop(0, heads // 2)
    def _(t):
        in_turn([backward(2 * t, 0), backward(2 * t + 1, 1), out_grad(t)])
        give(0, h_all.at[rows_tile(t), :], dwo_out.at[pl.ds(pl.multiple_of(my_col + t * QB, QB), QB), :])
        for a in (1, 2):
            for n in (2 * t, 2 * t + 1):
                give(a, res.at[a - 1, n], outs[a].at[:, head_cols(n)])

    def cols_of(j):
        return jnp.concatenate([res[j, n, here, :] for n in range(heads)], axis=1).T

    for j in range(3):
        cols_s[j] = cols_of(j)

    @pl.loop(0, model // MT)
    def _(d):
        r = pl.ds(pl.multiple_of(d * MT, MT), MT)
        dh_t = sum(nn(w3[j, r, :], cols_s[j]) for j in range(3))
        for k in range(CORES):
            dh_part[k, r, :] = dh_t[:, k * blk:(k + 1) * blk]

    dh_swap = swap_part(dh_part.at[other], dh_recv, 1)
    dh_swap.start()

    def finish_rows():
        a_swap.wait()
        a_out[...] = (a_part[mine, :] + a_recv[...]).astype(BF16)
        xhat, rstd = normalize(x_ref[...])
        dh_swap.wait()
        dh = (dh_part[core] + dh_recv[...]).T
        dl_buf[me] = jnp.sum(dh * xhat, axis=0, keepdims=True)
        small_send(dl_buf, dsem)
        dy = dh * ln_w
        dx = dy - jnp.mean(dy, axis=-1, keepdims=True) - xhat * jnp.mean(dy * xhat, axis=-1, keepdims=True)
        dx_out[...] = (dx * rstd).astype(BF16)

    @pl.loop(0, model // MT)
    def _(m):
        @pl.when(m == 2)
        def _():
            finish_rows()

        per = seq // MT
        place = pl.ds(pl.multiple_of(lax.rem(m, per) * MT, MT), MT)
        for part in range(0, heads, 4):
            gv = jnp.concatenate([res[2, part + n] for n in range(4)], axis=1)
            y = nn(wot_s[rows_tile(m, MT), :], gv).astype(BF16)
            for n in range(4):
                qkv[m // per, part + n, place, :] = y[:, n * HEAD_DIM:(n + 1) * HEAD_DIM]
        for n in range(heads):
            give(3, qkv.at[m // per, n, place, :], dwv_out.at[rows_tile(m, MT), head_cols(n)])

    ht_copy.wait()
    for kind, (block, piece, to) in sends.items():
        copy(1, kind, block, piece, to).wait_send()
    my_span = pl.ds(pl.multiple_of(core * width, width), width)
    their_span = pl.ds(pl.multiple_of(other * width, width), width)
    for a in range(4):
        sent = outs[a].at[my_span, :] if a == 0 else outs[a].at[:, my_span]
        came = outs[a].at[their_span, :] if a == 0 else outs[a].at[:, their_span]
        pltpu.make_async_copy(sent, sent, osem.at[a]).wait()
        done = pltpu.make_async_remote_copy(
            src_ref=sent, dst_ref=came, send_sem=xsem.at[0, a], recv_sem=xsem.at[1, a],
            device_id={"sp": partner}, device_id_type=MESH)
        done.wait_send()
        done.wait_recv()
    small_wait(dl_buf, dsem)
    total = dl_buf[0]
    for k in range(1, n_dev):
        total = total + dl_buf[k]
    dl_out[...] = total.astype(BF16).reshape(model)


def run_main(n_dev, hidden, d_attn, positions, ln_weight, w_q, w_k, w_v, w_o):
    blk, model = hidden.shape
    seq = n_dev * blk
    width = w_q.shape[1] // CORES
    heads = width // HEAD_DIM
    pairs = (seq // QB) * (seq // QB + 1) // 2
    vm = pl.BlockSpec(memory_space=pltpu.VMEM)
    hbm = pl.BlockSpec(memory_space=pl.ANY)
    full = w_q.shape[1]
    wide = jax.ShapeDtypeStruct((seq, full), BF16)
    rows = jax.ShapeDtypeStruct((blk, model), BF16)
    freq = np.repeat(ROPE_BASE ** (-np.arange(0, HEAD_DIM, 2) / HEAD_DIM), 2)[None, :].astype(np.float32)
    return pl.pallas_call(
        functools.partial(main_kernel, n_dev),
        out_shape=(jax.ShapeDtypeStruct((model, seq), BF16), jax.ShapeDtypeStruct((full, model), BF16),
                   wide, wide, jax.ShapeDtypeStruct((model, full), BF16), rows, rows, jax.ShapeDtypeStruct((model,), BF16)),
        in_specs=[vm] * 5 + [hbm] * 4,
        out_specs=[hbm] * 5 + [vm] * 3,
        scratch_shapes=[
            pltpu.VMEM((seq, model), BF16),
            pltpu.VMEM((seq, model), BF16),
            pltpu.VMEM((n_dev, 1, blk), jnp.int32),
            pltpu.VMEM((seq, HEAD_DIM), F32),
            pltpu.VMEM((seq, HEAD_DIM), F32),
            pltpu.VMEM((3, model, width), BF16),
            pltpu.VMEM((width, model), BF16),
            pltpu.VMEM((model, width), BF16),
            pltpu.VMEM((3, heads, seq, HEAD_DIM), BF16),
            pltpu.VMEM((heads, seq, HEAD_DIM), BF16),
            pltpu.VMEM((heads, HEAD_DIM, seq), BF16),
            pltpu.VMEM((3, heads, seq, HEAD_DIM), BF16),
            pltpu.VMEM((heads, 1, seq), F32),
            pltpu.VMEM((heads, 1, seq), F32),
            pltpu.VMEM((2, HEAD_DIM, seq), BF16),
            pltpu.VMEM((2, HEAD_DIM, seq), BF16),
            pltpu.VMEM((2, pairs, QB, QB), BF16),
            pltpu.VMEM((2, pairs, QB, QB), BF16),
            pltpu.VMEM((CORES * blk, model), F32),
            pltpu.VMEM((blk, model), F32),
            pltpu.VMEM((CORES, model, blk), F32),
            pltpu.VMEM((model, blk), F32),
            pltpu.VMEM((3, width, CORES * blk), BF16),
            pltpu.VMEM((n_dev, 1, model), F32),
            pltpu.SemaphoreType.DMA((2, 13)),
            pltpu.SemaphoreType.DMA((2, 13)),
            pltpu.SemaphoreType.DMA((4,)),
            pltpu.SemaphoreType.DMA((1,)),
            pltpu.SemaphoreType.DMA((2, 4)),
            pltpu.SemaphoreType.DMA((4,)),
            pltpu.SemaphoreType.DMA((2, n_dev)),
            pltpu.SemaphoreType.DMA((2, n_dev)),
            pltpu.SemaphoreType.DMA((2, 2)),
        ],
        compiler_params=pltpu.CompilerParams(
            collective_id=0, has_side_effects=True, vmem_limit_bytes=VMEM_LIMIT),
        name="gather_attention",
    )(hidden, d_attn, positions, freq, ln_weight, w_q, w_k, w_v, w_o)


def grad_kernel(ht, gq, gk, dwo_in, dwv_in, a_in, dx_in, dl_in,
                dq_out, dk_out, dwo_out, dwv_out, a_out, dx_out, dl_out,
                ht_v, g2, out_v, dwo_v, dwv_v, a_v, dx_v, hsem, gsem, usem, isem, osem, rsem):
    tiles = ht.shape[0] // MT
    steps = 2 * tiles
    wide = gq.shape[1]
    part = dwo_in.shape[0] // steps
    outs = (dq_out, dk_out)

    def rows(m, size=MT):
        return pl.ds(pl.multiple_of(m * size, size), size)

    ht_loads = [pltpu.make_async_copy(ht.at[rows(m), :], ht_v.at[rows(m), :], hsem.at[m]) for m in range(tiles)]
    g_loads = [pltpu.make_async_copy(x, g2.at[k], gsem.at[k]) for k, x in enumerate((gq, gk))]
    row_in = [pltpu.make_async_copy(a_in, a_v, rsem.at[0]), pltpu.make_async_copy(dx_in, dx_v, rsem.at[1])]
    row_out = [pltpu.make_async_copy(a_v, a_out, rsem.at[0]), pltpu.make_async_copy(dx_v, dx_out, rsem.at[1])]

    def bring(k, it):
        src, buf = ((dwo_in, dwo_v), (dwv_in, dwv_v))[k]
        return pltpu.make_async_copy(src.at[rows(it, part), :], buf.at[rows(it, part), :], isem.at[k, it])

    def put(k, it):
        buf, dst = ((dwo_v, dwo_out), (dwv_v, dwv_out))[k]
        return pltpu.make_async_copy(buf.at[rows(it, part), :], dst.at[rows(it, part), :], osem.at[k, it])

    def store(slot, out, m):
        return pltpu.make_async_copy(out_v.at[slot], out.at[rows(m), :], usem.at[slot])

    ht_loads[0].start()
    g_loads[0].start()
    for c in ht_loads[1:] + g_loads[1:] + row_in:
        c.start()
    for k in range(2):
        bring(k, 0).start()
    dl_out[...] = dl_in[...]

    @pl.loop(0, steps)
    def _(it):
        k, m, slot = it // tiles, lax.rem(it, tiles), lax.rem(it, 2)
        for j in range(tiles):
            @pl.when(it == j)
            def _():
                ht_loads[j].wait()
        for j in range(2):
            @pl.when(it == j * tiles)
            def _():
                g_loads[j].wait()

        @pl.when(it == 1)
        def _():
            for c, d in zip(row_in, row_out):
                c.wait()
                d.start()

        @pl.when(it >= 2)
        def _():
            store(slot, dq_out, 0).wait()

        for n in range(0, wide, NT):
            out_v[slot, :, n:n + NT] = nn(ht_v[rows(m), :], g2[k, :, n:n + NT]).astype(BF16)
        for j in range(2):
            @pl.when(k == j)
            def _():
                store(slot, outs[j], m).start()
            bring(j, it).wait()
            put(j, it).start()

            @pl.when(it < steps - 1)
            def _():
                bring(j, it + 1).start()

    for slot in range(2):
        store(slot, dq_out, 0).wait()
    for it in range(steps):
        for k in range(2):
            put(k, it).wait()
    for d in row_out:
        d.wait()


def run_grads(ht, dwo, gq, gk, dwv, attn_out, d_hid, d_lnw):
    model, seq = ht.shape
    wide = gq.shape[1]
    tiles = model // MT
    hbm = pl.BlockSpec(memory_space=pl.ANY)
    vm = pl.BlockSpec(memory_space=pltpu.VMEM)

    def like(a):
        return jax.ShapeDtypeStruct(a.shape, a.dtype)

    grad = jax.ShapeDtypeStruct((model, wide), BF16)
    return pl.pallas_call(
        grad_kernel,
        out_shape=[grad, grad, like(dwo), like(dwv), like(attn_out), like(d_hid), like(d_lnw)],
        in_specs=[hbm] * 7 + [vm],
        out_specs=[hbm] * 6 + [vm],
        scratch_shapes=[
            pltpu.VMEM((model, seq), BF16),
            pltpu.VMEM((2, seq, wide), BF16),
            pltpu.VMEM((2, MT, wide), BF16),
            pltpu.VMEM(dwo.shape, BF16),
            pltpu.VMEM(dwv.shape, BF16),
            pltpu.VMEM(attn_out.shape, BF16),
            pltpu.VMEM(d_hid.shape, BF16),
            pltpu.SemaphoreType.DMA((tiles,)),
            pltpu.SemaphoreType.DMA((2,)),
            pltpu.SemaphoreType.DMA((2,)),
            pltpu.SemaphoreType.DMA((2, 2 * tiles)),
            pltpu.SemaphoreType.DMA((2, 2 * tiles)),
            pltpu.SemaphoreType.DMA((2,)),
        ],
        compiler_params=pltpu.CompilerParams(vmem_limit_bytes=VMEM_LIMIT),
        name="weight_grads",
    )(ht, gq, gk, dwo, dwv, attn_out, d_hid, d_lnw)


def solution(mesh):
    n_dev = mesh.shape['sp']
    row_spec = P(('dp', 'sp'), None)
    full_spec = P(None, None)
    grad_spec = P('dp', None)

    def local_step(hidden, positions, d_attn, ln_weight, w_q, w_k, w_v, w_o):
        parts = run_main(n_dev, hidden, d_attn, positions, ln_weight, w_q, w_k, w_v, w_o)
        dwq, dwk, dwo, dwv, attn_out, d_hid, d_lnw = run_grads(*parts)
        return attn_out, d_hid, d_lnw, dwq, dwk, dwv, dwo

    return jax.shard_map(local_step, mesh=mesh,
                         in_specs=(row_spec, P(('dp', 'sp')), row_spec, P(None), full_spec, full_spec, full_spec, full_spec),
                         out_specs=(row_spec, row_spec, P('dp'), grad_spec, grad_spec, grad_spec, grad_spec),
                         check_vma=False)
```
